256 devices in a mesh: shot: 4 (over y_lo, core), space: 64 (over x, z, y_hi).
Axes of the slice: x: 4, y: 4 (y_hi: 2, y_lo: 2; y = y_hi * 2 + y_lo), z: 8, core: 2. Of those that a mesh axis runs over, the one named last changes fastest.
Arguments:
- adjoint_now: float32 [4, 1024, 64, 512], P('shot', 'space'), may hold values from -6 to 6
- adjoint_later: float32 [4, 1024, 64, 512], P('shot', 'space'), may hold values from -6 to 6
- courant: float32 [1024, 64, 512], P('space'), may hold values from 0.05 to 0.2
- checkpoint_codes: int32 [4, 6, 1024, 64, 128], P('shot', None, 'space'), may hold values from -2147483648 to 2147483646
- scale_index: int32 [4, 6, 1024, 256], P('shot', None, 'space'), may hold values from 0 to 63
- scale_table: float32 [64], replicated, may hold values from 0.001 to 0.01
- receiver_cell: int32 [4, 16384], P('shot', 'space'), may hold values from 0 to 33554431, as said below
- observed: float32 [4, 4, 16384], P('shot', None, 'space'), may hold values from -12 to 12
- source_cell: int32 [4, 3], P('shot'), may hold values from 0 to 1023, as said below
Outputs:
- gradient: float32 [1024, 64, 512], P('space', 'shot')
- adjoint_first: float32 [4, 1024, 64, 512], P('shot', 'space')
- adjoint_second: float32 [4, 1024, 64, 512], P('shot', 'space')
- misfit: float32 [], replicated
The draws below stay inside these ranges and needn't reach their ends.
Inputs may be any that keep to these rules, and one draw needn't show every extreme that they name: `receiver_cell`: for every r, entries r * 256 to (r + 1) * 256 - 1 of each shot's row are flat indices (z * 64 + y) * 512 + x of cells with r * 16 <= z < (r + 1) * 16. `source_cell`: column 0 is a z index below 1024, column 1 a y index below 64, column 2 an x index below 512.
All inputs are finite; a program needn't handle non-finite values.
Results may differ from the reference program's by a relative error of at most 0.0001.
Values sent between devices are 32-bit elements; how exact they have to be, the bound alone decides.
A program may use at most 128 MiB of HBM per device.

```python
import math
import jax
import jax.numpy as jnp

NX = 512
NY = 64
CZ = 16
ITERS = 4
QBLOCK = 128
SCALES = 64
MUTE = 8
REC_DEV = 256
LEVELS = 6
NZ = 1024
SHOTS = 4
RECEIVERS = 16384


def draw_receiver_cell(key, part):
    keys = jax.random.split(jax.random.fold_in(key, 11), 3)
    slab = jnp.arange(RECEIVERS, dtype=jnp.int32) // REC_DEV
    depth = slab * CZ + jax.random.randint(keys[0], (SHOTS, RECEIVERS), 0, CZ)
    row = jax.random.randint(keys[1], (SHOTS, RECEIVERS), 0, NY)
    col = jax.random.randint(keys[2], (SHOTS, RECEIVERS), 0, NX)
    return ((depth * NY + row) * NX + col).astype(jnp.int32)


def draw_observed(key, part):
    ramp = 1.0 + 2.0 * jnp.arange(RECEIVERS, dtype=jnp.float32) / RECEIVERS
    base = jnp.clip(jax.random.normal(jax.random.fold_in(key, 22), (SHOTS, ITERS, RECEIVERS), jnp.float32), -4.0, 4.0)
    return (base * ramp).astype(jnp.float32)


def draw_source_cell(key, part):
    keys = jax.random.split(jax.random.fold_in(key, 31), 4)
    depth = jax.random.randint(keys[0], (SHOTS, 1), 0, NZ)
    row = jax.random.randint(keys[1], (SHOTS, 1), 0, NY)
    col = jax.random.randint(keys[2], (SHOTS, 1), 0, NX)
    chosen = jax.random.randint(keys[3], (), 0, SHOTS)
    marked = (jnp.arange(SHOTS, dtype=jnp.int32) == chosen).reshape(SHOTS, 1)
    depth = jnp.where(marked, NZ - 1, depth)
    row = jnp.where(marked, 0, row)
    return jnp.concatenate([depth, row, col], axis=1).astype(jnp.int32)


def set_ends(entries, key, smallest, largest):
    index_at = [jax.random.randint(jax.random.fold_in(key, axis), (), 0, length) for axis, length in enumerate(entries.shape)]
    longest = entries.shape.index(max(entries.shape))
    neighbour = index_at[:longest] + [(index_at[longest] + 1) % entries.shape[longest]] + index_at[longest + 1:]
    return entries.at[tuple(index_at)].set(smallest).at[tuple(neighbour)].set(largest)


def block_scale(rng, dims, cuts, low, high):
    loudness = 1.0
    for dim, parts in cuts:
        draws = jax.random.uniform(jax.random.fold_in(jax.random.fold_in(rng, 6), dim), (parts,), jnp.float32, low / len(cuts), high / len(cuts))
        loudness = loudness * jnp.repeat(jnp.exp(draws), dims[dim] // parts).reshape((-1,) + (1,) * (len(dims) - 1 - dim))
    return loudness


def scatter_about(key, shape, width, limit, shards=(), kind=jnp.bfloat16):
    gain = block_scale(key, shape, shards, -0.22, 0.18) if shards else 1.0
    values = jax.random.normal(key, shape, jnp.float32) * width * gain
    return jnp.minimum(jnp.maximum(values, -limit), limit).astype(kind)


def setup_inputs(seed: int = 0) -> dict:
    seeds = jax.random.split(jax.random.key(seed), 10)
    return {
        "adjoint_now": scatter_about(seeds[0], (SHOTS, NZ, NY, NX), 1.0, 6.0, ((0, 4), (1, 64)), jnp.float32),
        "adjoint_later": scatter_about(seeds[1], (SHOTS, NZ, NY, NX), 1.0, 6.0, ((0, 4), (1, 64)), jnp.float32),
        "courant": jnp.clip(jnp.exp(math.log(0.2) - 1.3862944 * jax.random.uniform(seeds[2], (NZ, NY, NX), jnp.float32) ** block_scale(seeds[2], (NZ, NY, NX), ((0, 64),), -0.2, 0.2)), 0.05, 0.2),
        "checkpoint_codes": set_ends(jax.random.randint(seeds[3], (SHOTS, LEVELS, NZ, NY, NX // 4), -2147483648, 2147483647), jax.random.fold_in(seeds[3], 1), -2147483648, 2147483646).astype(jnp.int32),
        "scale_index": set_ends(jax.random.randint(seeds[4], (SHOTS, LEVELS, NZ, NY * NX // QBLOCK), 0, SCALES), jax.random.fold_in(seeds[4], 1), 0, SCALES - 1).astype(jnp.int32),
        "scale_table": jnp.clip(jnp.exp(jax.random.uniform(seeds[5], (SCALES,), jnp.float32, math.log(0.001), math.log(0.01))), 0.001, 0.01),
        "receiver_cell": draw_receiver_cell(jax.random.fold_in(seeds[9], 71), 0),
        "observed": draw_observed(jax.random.fold_in(seeds[9], 71), 0),
        "source_cell": draw_source_cell(jax.random.fold_in(seeds[9], 71), 0),
    }


COEFFS = (-205.0 / 72.0, 8.0 / 5.0, -1.0 / 5.0, 8.0 / 315.0, -1.0 / 560.0)


def decode(words, index, table):
    planes = [jnp.bitwise_and(jnp.right_shift(words, 8 * m), 255) for m in range(4)]
    codes = jnp.concatenate(planes, axis=-1)
    centred = (codes - 128).astype(jnp.float32)
    depth, rows, cols = centred.shape
    scale = table[index]
    blocks = centred.reshape(depth, rows, cols // QBLOCK, QBLOCK) * scale.reshape(depth, rows, cols // QBLOCK, 1)
    return blocks.reshape(depth, rows, cols)


def laplace(field):
    padded = jnp.pad(field, 4)
    depth, rows, cols = field.shape
    total = 3.0 * COEFFS[0] * field
    for step in range(1, 5):
        total = total + COEFFS[step] * (padded[4 + step:4 + step + depth, 4:4 + rows, 4:4 + cols] + padded[4 - step:4 - step + depth, 4:4 + rows, 4:4 + cols])
        total = total + COEFFS[step] * (padded[4:4 + depth, 4 + step:4 + step + rows, 4:4 + cols] + padded[4:4 + depth, 4 - step:4 - step + rows, 4:4 + cols])
        total = total + COEFFS[step] * (padded[4:4 + depth, 4:4 + rows, 4 + step:4 + step + cols] + padded[4:4 + depth, 4:4 + rows, 4 - step:4 - step + cols])
    return total


def reference(adjoint_now, adjoint_later, courant, checkpoint_codes, scale_index, scale_table, receiver_cell, observed, source_cell):
    gradient = jnp.zeros((NZ, NY, NX), jnp.float32)
    misfit_sum = jnp.zeros((), jnp.float32)
    firsts = []
    seconds = []
    zpos = jnp.arange(NZ, dtype=jnp.int32).reshape(NZ, 1, 1)
    ypos = jnp.arange(NY, dtype=jnp.int32).reshape(1, NY, 1)
    xpos = jnp.arange(NX, dtype=jnp.int32).reshape(1, 1, NX)
    for shot in range(SHOTS):
        fields = [decode(checkpoint_codes[shot, level], scale_index[shot, level], scale_table) for level in range(ITERS + 2)]
        now = adjoint_now[shot]
        later = adjoint_later[shot]
        image = jnp.zeros((NZ, NY, NX), jnp.float32)
        cells = receiver_cell[shot]
        for step in range(ITERS):
            level = ITERS - step
            synthetic = jnp.take(fields[level].reshape(-1), cells)
            residual = synthetic - observed[shot, level - 1]
            misfit_sum = misfit_sum + jnp.sum(residual * residual)
            image = image + now * (fields[level + 1] - 2.0 * fields[level] + fields[level - 1])
            stepped = 2.0 * now - later + courant * laplace(now)
            stepped = stepped.reshape(-1).at[cells].add(residual).reshape(NZ, NY, NX)
            later = now
            now = stepped
        source = source_cell[shot]
        dist = ((zpos - source[0]) ** 2 + (ypos - source[1]) ** 2 + (xpos - source[2]) ** 2).astype(jnp.float32)
        mute = 1.0 - jnp.exp(-dist / (2.0 * MUTE * MUTE))
        gradient = gradient + image * mute
        firsts.append(now)
        seconds.append(later)
    misfit = 0.5 * misfit_sum / (SHOTS * ITERS * RECEIVERS)
    return gradient, jnp.stack(firsts), jnp.stack(seconds), misfit
```

```python
import functools

import jax
import jax.numpy as jnp
from jax import lax
from jax.experimental import pallas as pl
from jax.experimental.pallas import tpu as pltpu
from jax.sharding import PartitionSpec as P

STEPS = 4
MUTE = 8
RADIUS = 4
LANES = 128
PAD = 8
CHUNKS = 4
COEFFS = (-205.0 / 72.0, 8.0 / 5.0, -1.0 / 5.0, 8.0 / 315.0, -1.0 / 560.0)
MESH = pl.DeviceIdType.MESH


def kernel(
    space_size,
    shot_size,
    table,
    source,
    now_hbm,
    later_hbm,
    courant_hbm,
    codes_hbm,
    index_hbm,
    cells_hbm,
    observed_hbm,
    grad_hbm,
    first_hbm,
    second_hbm,
    misfit_hbm,
    field,
    courant,
    words,
    index,
    cells,
    observed,
    scales,
    flipped,
    spread,
    rows_hot,
    cols_hot,
    values,
    injected,
    image,
    from_sibling,
    combined,
    from_partner,
    grad_out,
    sums,
    sums_in,
    load_sem,
    out_sem,
    halo_send,
    halo_recv,
    image_send,
    image_recv,
    sum_send,
    sum_recv,
):
    depth = courant.shape[1]
    height = courant.shape[2]
    tall = height // CHUNKS
    receivers = cells.shape[1]
    me = lax.axis_index("space")
    shot = lax.axis_index("shot")
    side, core = shot // 2, shot % 2
    up, down = (me + 1) % space_size, (me + space_size - 1) % space_size
    sibling = shot + 1 - 2 * core
    partner = (shot + 2) % 4

    loads = []

    def load(src, dst):
        copy = pltpu.make_async_copy(src, dst, load_sem.at[len(loads)])
        copy.start()
        loads.append(copy)
        return copy

    def lanes(xc):
        return pl.ds(xc * LANES, LANES)

    edges = []
    for xc in range(4):
        for z in (0, depth - RADIUS):
            edges.append(
                load(
                    now_hbm.at[0, pl.ds(z, RADIUS), :, lanes(xc)],
                    field.at[1, xc, pl.ds(RADIUS + z, RADIUS), pl.ds(PAD, height), :],
                )
            )
    small = [
        load(index_hbm.at[0], index),
        load(cells_hbm, cells),
        load(observed_hbm.at[0], observed),
    ]
    small_words = load(codes_hbm.at[0], words)
    rest = []
    for xc in range(4):
        rest.append(
            load(
                now_hbm.at[0, pl.ds(RADIUS, depth - 2 * RADIUS), :, lanes(xc)],
                field.at[1, xc, pl.ds(2 * RADIUS, depth - 2 * RADIUS), pl.ds(PAD, height), :],
            )
        )
        rest.append(
            load(
                later_hbm.at[0, :, :, lanes(xc)],
                field.at[0, xc, pl.ds(RADIUS, depth), pl.ds(PAD, height), :],
            )
        )
        rest.append(load(courant_hbm.at[:, :, lanes(xc)], courant.at[xc]))

    def flip(i, bit):
        return i + bit - 2 * bit * ((i // bit) % 2)

    stages = []
    bit = 1
    while bit < space_size:
        stages.append({"space": flip(me, bit)})
        bit *= 2
    bit = 1
    while bit < shot_size:
        stages.append({"shot": flip(shot, bit)})
        bit *= 2
    peers = stages + [{"space": up}, {"space": down}]
    barrier = pltpu.get_barrier_semaphore()
    for peer in peers:
        pl.semaphore_signal(barrier, inc=1, device_id=peer, device_id_type=MESH)

    zero_rows = jnp.zeros((4, 1, PAD, LANES), jnp.float32)

    def clear_rows(i, carry):
        level = 1 + i // depth
        z = RADIUS + i % depth
        field[pl.ds(level, 1), :, pl.ds(z, 1), pl.ds(0, PAD), :] = zero_rows[None]
        field[pl.ds(level, 1), :, pl.ds(z, 1), pl.ds(PAD + height, PAD), :] = zero_rows[None]
        return carry

    lax.fori_loop(0, STEPS * depth, clear_rows, 0)
    zero_plane = jnp.zeros((1, 4, 1, height, LANES), jnp.float32)

    @pl.when(me == 0)
    def _():
        def clear(i, carry):
            field[pl.ds(1 + i // RADIUS, 1), :, pl.ds(i % RADIUS, 1), pl.ds(PAD, height), :] = (
                zero_plane
            )
            return carry

        lax.fori_loop(0, STEPS * RADIUS, clear, 0)

    @pl.when(me == space_size - 1)
    def _():
        def clear(i, carry):
            field[
                pl.ds(1 + i // RADIUS, 1),
                :,
                pl.ds(RADIUS + depth + i % RADIUS, 1),
                pl.ds(PAD, height),
                :,
            ] = zero_plane
            return carry

        lax.fori_loop(0, STEPS * RADIUS, clear, 0)

    pl.semaphore_wait(barrier, len(peers))

    def rows_of(n):
        c = (n + 2 * (1 - side)) % CHUNKS
        return c, pl.multiple_of(PAD + c * tall, 8)

    def halo_copy(t, n, way):
        _, row = rows_of(n)
        src_z, dst_z, target = ((depth, 0, up), (RADIUS, RADIUS + depth, down))[way]
        return pltpu.make_async_remote_copy(
            src_ref=field.at[1 + t, :, pl.ds(src_z, RADIUS), pl.ds(row, tall), :],
            dst_ref=field.at[1 + t, :, pl.ds(dst_z, RADIUS), pl.ds(row, tall), :],
            send_sem=halo_send.at[way, t, n],
            recv_sem=halo_recv.at[way, t, n],
            device_id={"space": target},
            device_id_type=MESH,
        )

    has_up = me < space_size - 1
    has_down = me > 0

    def send_halo(t, n):
        @pl.when(has_up)
        def _():
            halo_copy(t, n, 0).start()

        @pl.when(has_down)
        def _():
            halo_copy(t, n, 1).start()

    def wait_halo(t, n):
        @pl.when(has_down)
        def _():
            halo_copy(t, n, 0).wait_recv()

        @pl.when(has_up)
        def _():
            halo_copy(t, n, 1).wait_recv()

    for copy in edges:
        copy.wait()

    def first_sends(n, carry):
        send_halo(0, n)
        return carry

    lax.fori_loop(0, CHUNKS, first_sends, 0)

    for copy in small:
        copy.wait()
    levels = index.shape[0]
    flat_index = index[...].reshape(levels * depth, index.shape[2])

    def look_up(k, acc):
        return jnp.where(flat_index == k, table[k], acc)

    looked = lax.fori_loop(0, table.shape[0], look_up, jnp.zeros(flat_index.shape, jnp.float32))
    scales[pl.ds(0, levels * depth), :] = looked
    scales[pl.ds(levels * depth, LANES - levels * depth), :] = jnp.zeros(
        (LANES - levels * depth, index.shape[2]), jnp.float32
    )
    flipped[...] = scales[...].T
    columns = [flipped[pl.ds(m, height, stride=4), :] for m in range(4)]

    def spread_one(i, carry):
        level, z = i // depth, i % depth
        for m in range(4):
            moved = pltpu.roll(columns[m], LANES - i, 1)
            spread[pl.ds(level, 1), pl.ds(z, 1), m, :, :] = jnp.broadcast_to(
                moved[:, 0:1], (height, LANES)
            )[None, None]
        return carry

    for m in range(4):
        spread[0, 0, m, :, :] = jnp.broadcast_to(columns[m][:, 0:1], (height, LANES))
    lax.fori_loop(1, levels * depth, spread_one, 0)

    width = 4 * LANES
    cell = cells[...] - me * (depth * height * width)
    row_of = cell // width
    col_of = cell % width
    block_of = (cell // LANES) % (4 * height)
    slab_of = row_of // height
    for z in range(depth):
        ids = z * height + lax.broadcasted_iota(jnp.int32, (height, receivers), 0)
        rows_hot[z] = jnp.where(ids == row_of, 1.0, 0.0).astype(jnp.bfloat16)
    col_ids = lax.broadcasted_iota(jnp.int32, (width, receivers), 0)
    cols_hot[...] = jnp.where(col_ids == col_of, 1.0, 0.0).astype(jnp.bfloat16)
    block_ids = lax.broadcasted_iota(jnp.int32, (4 * height, receivers), 0)
    blocks_hot = jnp.where(block_ids == block_of, 1.0, 0.0)
    scale_at = jnp.dot(
        scales[...], blocks_hot, precision=lax.Precision.HIGHEST, preferred_element_type=jnp.float32
    )
    depth_ids = lax.broadcasted_iota(jnp.int32, (depth, receivers), 0)
    small_words.wait()
    planes = 4
    total = jnp.zeros((1, receivers), jnp.float32)
    for t in range(STEPS):
        level = STEPS - t

        def gather(i, acc):
            w = words[level, pl.ds(i * planes, planes), :, :].reshape(planes * height, LANES)
            parts = [
                (((w >> (8 * m)) & 255) - 128).astype(jnp.float32).astype(jnp.bfloat16)
                for m in range(4)
            ]
            found = jnp.dot(
                jnp.concatenate(parts, axis=1), cols_hot[...], preferred_element_type=jnp.float32
            )
            hot = rows_hot[pl.ds(i * planes, planes), :, :].reshape(planes * height, receivers)
            return acc + jnp.sum(found * hot.astype(jnp.float32), axis=0, keepdims=True)

        code = lax.fori_loop(
            0, depth // planes, gather, jnp.zeros((1, receivers), jnp.float32)
        )
        part = scale_at[level * depth : (level + 1) * depth]
        scale = jnp.sum(jnp.where(depth_ids == slab_of, part, 0.0), axis=0, keepdims=True)
        residual = code * scale - observed[level - 1 : level, :]
        total = total + residual * residual
        left = residual
        for piece in range(3):
            short = left.astype(jnp.bfloat16).astype(jnp.float32)
            left = left - short
            values[t, piece] = jnp.where(col_ids == col_of, short, 0.0).astype(jnp.bfloat16)
    sums[0] = jnp.broadcast_to(
        jnp.sum(total, axis=1, keepdims=True), sums.shape[1:]
    )

    def sum_copy(b):
        return pltpu.make_async_remote_copy(
            src_ref=sums.at[b],
            dst_ref=sums_in.at[b],
            send_sem=sum_send.at[b],
            recv_sem=sum_recv.at[b],
            device_id=stages[b],
            device_id_type=MESH,
        )

    for copy in rest:
        copy.wait()

    lane = lax.broadcasted_iota(jnp.int32, (tall, LANES), 1)

    def update(t, c, row, z):
        def at(xc, dz, dy):
            return field[1 + t, xc, RADIUS + z + dz, pl.ds(row + dy, tall), :]

        centre = [at(xc, 0, 0) for xc in range(4)]
        after = [[pltpu.roll(v, LANES - i, 1) for v in centre] for i in range(1, 5)]
        before = [[pltpu.roll(v, i, 1) for v in centre] for i in range(1, 5)]
        for xc in range(4):
            acc = (3.0 * COEFFS[0]) * centre[xc]
            for i in range(1, 5):
                nxt = after[i - 1][xc + 1] if xc < 3 else 0.0
                prv = before[i - 1][xc - 1] if xc > 0 else 0.0
                pair = jnp.where(lane < LANES - i, after[i - 1][xc], nxt) + jnp.where(
                    lane >= i, before[i - 1][xc], prv
                )
                pair = pair + (at(xc, i, 0) + at(xc, -i, 0)) + (at(xc, 0, i) + at(xc, 0, -i))
                acc = acc + COEFFS[i] * pair
            y0 = pl.multiple_of(row - PAD, 8)
            old = field[t, xc, RADIUS + z, pl.ds(row, tall), :]
            new = 2.0 * centre[xc] - old + courant[xc, z, pl.ds(y0, tall), :] * acc
            field[2 + t, xc, RADIUS + z, pl.ds(row, tall), :] = new + injected[xc, z, :, :]

    def inject(t, c):
        hot = rows_hot[:, pl.ds(pl.multiple_of(c * tall, 16), tall), :].reshape(
            depth * tall, receivers
        )
        acc = None
        for piece in range(3):
            term = lax.dot_general(
                hot,
                values[t, piece],
                (((1,), (1,)), ((), ())),
                preferred_element_type=jnp.float32,
            )
            acc = term if acc is None else acc + term
        for xc in range(4):
            injected[xc] = acc[:, xc * LANES : (xc + 1) * LANES].reshape(depth, tall, LANES)

    def add_image(t, c, row, first):
        level = STEPS - t
        y0 = pl.multiple_of(row - PAD, 8)

        def plane(z, carry):
            ws = [words[level + d, z, pl.ds(y0, tall), :] for d in (-1, 0, 1)]
            for m in range(4):
                f = [
                    (((w >> (8 * m)) & 255) - 128).astype(jnp.float32)
                    * spread[level + d, z, m, pl.ds(y0, tall), :]
                    for w, d in zip(ws, (-1, 0, 1))
                ]
                term = field[1 + t, m, RADIUS + z, pl.ds(row, tall), :] * (
                    f[2] - 2.0 * f[1] + f[0]
                )
                if first:
                    image[c, m, z] = term
                else:
                    image[c, m, z] = image[c, m, z] + term
            return carry

        lax.fori_loop(0, depth, plane, 0)

    def mute(c):
        y = c * tall + lax.broadcasted_iota(jnp.int32, (tall, LANES), 0)
        across = [(y - source[1]) ** 2 + (m * LANES + lane - source[2]) ** 2 for m in range(4)]

        def plane(z, carry):
            dz = me * depth + z - source[0]
            for m in range(4):
                dist = (across[m] + dz * dz).astype(jnp.float32)
                image[c, m, z] = image[c, m, z] * (1.0 - jnp.exp(-dist / (2.0 * MUTE * MUTE)))
            return carry

        lax.fori_loop(0, depth, plane, 0)

    far = 2 * (1 - side) + core
    near = shot

    def pair_copy(c, slot):
        return pltpu.make_async_remote_copy(
            src_ref=image.at[c],
            dst_ref=from_sibling.at[slot],
            send_sem=image_send.at[slot],
            recv_sem=image_recv.at[slot],
            device_id={"shot": sibling},
            device_id_type=MESH,
        )

    sibling_far = 2 * (1 - side) + 1 - core
    far_copy = pair_copy(sibling_far, 0)
    near_copy = pair_copy(sibling, 1)
    partner_copy = pltpu.make_async_remote_copy(
        src_ref=combined,
        dst_ref=from_partner,
        send_sem=image_send.at[2],
        recv_sem=image_recv.at[2],
        device_id={"shot": partner},
        device_id_type=MESH,
    )

    outs = []

    def store(src, dst):
        copy = pltpu.make_async_copy(src, dst, out_sem.at[len(outs)])
        copy.start()
        outs.append(copy)

    def first_copy(n, xc):
        c, row = rows_of(n)
        return pltpu.make_async_copy(
            field.at[1 + STEPS, xc, pl.ds(RADIUS, depth), pl.ds(row, tall), :],
            first_hbm.at[0, :, pl.ds(pl.multiple_of(row - PAD, 8), tall), lanes(xc)],
            out_sem.at[16 + n * 4 + xc],
        )

    for t in range(STEPS):

        def task(n, carry, t=t):
            c, row = rows_of(n)
            if t < 2:
                for j in range(4):
                    b = 4 * t + j

                    @pl.when(n == j)
                    def _():
                        if b > 0:
                            sum_copy(b - 1).wait_recv()
                            sums[b] = sums[b - 1] + sums_in[b - 1]
                        sum_copy(b).start()

            inject(t, c)

            def inner(z, carry):
                update(t, c, row, z)
                return carry

            lax.fori_loop(RADIUS, depth - RADIUS, inner, 0)
            if t == 0:
                add_image(0, c, row, True)
            if t == 2:

                @pl.when(n == 2)
                def _():
                    far_copy.wait_recv()

                    def plane(z, carry):
                        for m in range(4):
                            combined[m, z] = image[far, m, z] + from_sibling[0, m, z]
                        return carry

                    lax.fori_loop(0, depth, plane, 0)
                    partner_copy.start()

            if t == 3:

                @pl.when(n == 3)
                def _():
                    near_copy.wait_recv()
                    partner_copy.wait_recv()

                    def plane(z, carry):
                        for m in range(4):
                            grad_out[m, z] = (
                                image[near, m, z] + from_sibling[1, m, z] + from_partner[m, z]
                            )
                        return carry

                    lax.fori_loop(0, depth, plane, 0)

            wait_halo(t, n)

            def outer(z, carry):
                update(t, c, row, z)
                update(t, c, row, depth - RADIUS + z)
                return carry

            lax.fori_loop(0, RADIUS, outer, 0)
            if t < STEPS - 1:
                send_halo(t + 1, n)
                add_image(t + 1, c, row, False)
            else:
                for xc in range(4):
                    first_copy(n, xc).start()
            if t == 2:
                mute(c)

                @pl.when(c == sibling_far)
                def _():
                    far_copy.start()

                @pl.when(c == sibling)
                def _():
                    near_copy.start()

            return carry

        lax.fori_loop(0, CHUNKS, task, 0)
        if t == 1:
            last = len(stages) - 1
            sum_copy(last).wait_recv()
            sums[last + 1] = sums[last] + sums_in[last]
        if t == 2:
            for xc in range(4):
                store(
                    field.at[STEPS, xc, pl.ds(RADIUS, depth), pl.ds(PAD, height), :],
                    second_hbm.at[0, :, :, lanes(xc)],
                )
            store(sums.at[len(stages)], misfit_hbm)
    for xc in range(4):
        store(grad_out.at[xc], grad_hbm.at[:, :, lanes(xc)])

    def drain(n, carry):
        for t in range(STEPS):

            @pl.when(has_up)
            def _():
                halo_copy(t, n, 0).wait_send()

            @pl.when(has_down)
            def _():
                halo_copy(t, n, 1).wait_send()

        for xc in range(4):
            first_copy(n, xc).wait()
        return carry

    far_copy.wait_send()
    near_copy.wait_send()
    partner_copy.wait_send()
    for b in range(len(stages)):
        sum_copy(b).wait_send()
    lax.fori_loop(0, CHUNKS, drain, 0)
    for copy in outs:
        copy.wait()


def body(
    space_size,
    shot_size,
    adjoint_now,
    adjoint_later,
    courant,
    checkpoint_codes,
    scale_index,
    scale_table,
    receiver_cell,
    observed,
    source_cell,
):
    _, depth, height, width = adjoint_now.shape
    levels = checkpoint_codes.shape[1]
    receivers = receiver_cell.shape[1]
    tall = height // CHUNKS
    quarter = (4, depth, tall, LANES)
    stages = (space_size * shot_size).bit_length() - 1
    whole = pl.BlockSpec(memory_space=pl.ANY)
    scalars = pl.BlockSpec(memory_space=pltpu.SMEM)
    f32 = jnp.float32
    gradient, first, second, misfit = pl.pallas_call(
        functools.partial(kernel, space_size, shot_size),
        out_shape=(
            jax.ShapeDtypeStruct((depth, tall, width), f32),
            jax.ShapeDtypeStruct(adjoint_now.shape, f32),
            jax.ShapeDtypeStruct(adjoint_now.shape, f32),
            jax.ShapeDtypeStruct((8, LANES), f32),
        ),
        in_specs=[scalars, scalars] + [whole] * 7,
        out_specs=[whole] * 4,
        scratch_shapes=[
            pltpu.VMEM((STEPS + 2, 4, depth + 2 * RADIUS, height + 2 * PAD, LANES), f32),
            pltpu.VMEM((4, depth, height, LANES), f32),
            pltpu.VMEM((levels, depth, height, LANES), jnp.int32),
            pltpu.VMEM((levels, depth, 4 * height), jnp.int32),
            pltpu.VMEM((1, receivers), jnp.int32),
            pltpu.VMEM((STEPS, receivers), f32),
            pltpu.VMEM((LANES, 4 * height), f32),
            pltpu.VMEM((4 * height, LANES), f32),
            pltpu.VMEM((levels, depth, 4, height, LANES), f32),
            pltpu.VMEM((depth, height, receivers), jnp.bfloat16),
            pltpu.VMEM((width, receivers), jnp.bfloat16),
            pltpu.VMEM((STEPS, 3, width, receivers), jnp.bfloat16),
            pltpu.VMEM(quarter, f32),
            pltpu.VMEM((CHUNKS, *quarter), f32),
            pltpu.VMEM((2, *quarter), f32),
            pltpu.VMEM(quarter, f32),
            pltpu.VMEM(quarter, f32),
            pltpu.VMEM(quarter, f32),
            pltpu.VMEM((stages + 1, 8, LANES), f32),
            pltpu.VMEM((stages, 8, LANES), f32),
            pltpu.SemaphoreType.DMA((32,)),
            pltpu.SemaphoreType.DMA((32,)),
            pltpu.SemaphoreType.DMA((2, STEPS, CHUNKS)),
            pltpu.SemaphoreType.DMA((2, STEPS, CHUNKS)),
            pltpu.SemaphoreType.DMA((3,)),
            pltpu.SemaphoreType.DMA((3,)),
            pltpu.SemaphoreType.DMA((stages,)),
            pltpu.SemaphoreType.DMA((stages,)),
        ],
        compiler_params=pltpu.CompilerParams(
            collective_id=0, has_side_effects=True, vmem_limit_bytes=60 * 1024 * 1024
        ),
    )(
        scale_table,
        source_cell[0],
        adjoint_now,
        adjoint_later,
        courant,
        checkpoint_codes,
        scale_index,
        receiver_cell,
        observed,
    )
    count = shot_size * STEPS * receivers * space_size
    return gradient, first, second, 0.5 * misfit[0, 0] / count


def solution(mesh):
    sizes = dict(mesh.shape)
    return jax.shard_map(
        functools.partial(body, sizes["space"], sizes["shot"]),
        mesh=mesh,
        in_specs=(
            P("shot", "space", None, None),
            P("shot", "space", None, None),
            P("space", None, None),
            P("shot", None, "space", None, None),
            P("shot", None, "space", None),
            P(),
            P("shot", "space"),
            P("shot", None, "space"),
            P("shot", None),
        ),
        out_specs=(
            P("space", "shot", None),
            P("shot", "space", None, None),
            P("shot", "space", None, None),
            P(),
        ),
        check_vma=False,
    )
```

```python
import functools

import jax
import jax.numpy as jnp
from jax import lax
from jax.experimental import pallas as pl
from jax.experimental.pallas import tpu as pltpu
from jax.sharding import PartitionSpec as P

STEPS = 4
MUTE = 8
RADIUS = 4
LANES = 128
PAD = 8
CHUNKS = 4
COEFFS = (-205.0 / 72.0, 8.0 / 5.0, -1.0 / 5.0, 8.0 / 315.0, -1.0 / 560.0)
MESH = pl.DeviceIdType.MESH


def kernel(
    space_size,
    shot_size,
    now_hbm,
    later_hbm,
    courant_hbm,
    codes_hbm,
    index_hbm,
    cells_hbm,
    observed_hbm,
    table_hbm,
    source_hbm,
    grad_hbm,
    first_hbm,
    second_hbm,
    misfit_hbm,
    table,
    source_ref,
    field,
    courant,
    words,
    index,
    cells,
    observed,
    scales,
    flipped,
    spread,
    rows_hot,
    cols_hot,
    values,
    injected,
    image,
    from_sibling,
    combined,
    from_partner,
    grad_out,
    sums,
    sums_in,
    load_sem,
    out_sem,
    halo_send,
    halo_recv,
    image_send,
    image_recv,
    sum_send,
    sum_recv,
):
    scale = 0.5 / (shot_size * STEPS * cells.shape[1] * space_size)
    depth = courant.shape[1]
    height = courant.shape[2]
    tall = height // CHUNKS
    receivers = cells.shape[1]
    me = lax.axis_index("space")
    shot = lax.axis_index("shot")
    side, core = shot // 2, shot % 2
    up, down = (me + 1) % space_size, (me + space_size - 1) % space_size
    sibling = shot + 1 - 2 * core
    partner = (shot + 2) % 4

    def flip(i, bit):
        return i + bit - 2 * bit * ((i // bit) % 2)

    stages = []
    bit = 1
    while bit < space_size:
        stages.append({"space": flip(me, bit)})
        bit *= 2
    bit = 1
    while bit < shot_size:
        stages.append({"shot": flip(shot, bit)})
        bit *= 2
    peers = stages + [{"space": up}, {"space": down}]
    barrier = pltpu.get_barrier_semaphore()
    for peer in peers:
        pl.semaphore_signal(barrier, inc=1, device_id=peer, device_id_type=MESH)

    loads = []

    def load(src, dst):
        copy = pltpu.make_async_copy(src, dst, load_sem.at[len(loads)])
        copy.start()
        loads.append(copy)
        return copy

    def lanes(xc):
        return pl.ds(xc * LANES, LANES)

    edges = []
    for xc in range(4):
        for z in (0, depth - RADIUS):
            edges.append(
                load(
                    now_hbm.at[0, pl.ds(z, RADIUS), :, lanes(xc)],
                    field.at[1, xc, pl.ds(RADIUS + z, RADIUS), pl.ds(PAD, height), :],
                )
            )
    small = [
        load(index_hbm.at[0], index),
        load(cells_hbm, cells),
        load(observed_hbm.at[0], observed),
        load(table_hbm, table),
        load(source_hbm, source_ref),
    ]
    small_words = load(codes_hbm.at[0], words)
    rest = []
    for xc in range(4):
        rest.append(
            load(
                now_hbm.at[0, pl.ds(RADIUS, depth - 2 * RADIUS), :, lanes(xc)],
                field.at[1, xc, pl.ds(2 * RADIUS, depth - 2 * RADIUS), pl.ds(PAD, height), :],
            )
        )
        rest.append(
            load(
                later_hbm.at[0, :, :, lanes(xc)],
                field.at[0, xc, pl.ds(RADIUS, depth), pl.ds(PAD, height), :],
            )
        )
        rest.append(load(courant_hbm.at[:, :, lanes(xc)], courant.at[xc]))

    pl.semaphore_wait(barrier, len(peers))

    def rows_of(n):
        c = (n + 2 * (1 - side)) % CHUNKS
        return c, pl.multiple_of(PAD + c * tall, 8)

    def halo_copy(t, n, way):
        _, row = rows_of(n)
        src_z, dst_z, target = ((depth, 0, up), (RADIUS, RADIUS + depth, down))[way]
        return pltpu.make_async_remote_copy(
            src_ref=field.at[1 + t, :, pl.ds(src_z, RADIUS), pl.ds(row, tall), :],
            dst_ref=field.at[1 + t, :, pl.ds(dst_z, RADIUS), pl.ds(row, tall), :],
            send_sem=halo_send.at[way, t, n],
            recv_sem=halo_recv.at[way, t, n],
            device_id={"space": target},
            device_id_type=MESH,
        )

    has_up = me < space_size - 1
    has_down = me > 0

    def send_halo(t, n):
        @pl.when(has_up)
        def _():
            halo_copy(t, n, 0).start()

        @pl.when(has_down)
        def _():
            halo_copy(t, n, 1).start()

    for copy in edges:
        copy.wait()

    def first_sends(n, carry):
        send_halo(0, n)
        return carry

    lax.fori_loop(0, CHUNKS, first_sends, 0)

    zero_rows = jnp.zeros((4, 1, PAD, LANES), jnp.float32)

    def clear_rows(i, carry):
        level = 1 + i // depth
        z = RADIUS + i % depth
        field[pl.ds(level, 1), :, pl.ds(z, 1), pl.ds(0, PAD), :] = zero_rows[None]
        field[pl.ds(level, 1), :, pl.ds(z, 1), pl.ds(PAD + height, PAD), :] = zero_rows[None]
        return carry

    lax.fori_loop(0, STEPS * depth, clear_rows, 0)
    zero_plane = jnp.zeros((1, 4, 1, height, LANES), jnp.float32)

    @pl.when(me == 0)
    def _():
        def clear(i, carry):
            field[pl.ds(1 + i // RADIUS, 1), :, pl.ds(i % RADIUS, 1), pl.ds(PAD, height), :] = (
                zero_plane
            )
            return carry

        lax.fori_loop(0, STEPS * RADIUS, clear, 0)

    @pl.when(me == space_size - 1)
    def _():
        def clear(i, carry):
            field[
                pl.ds(1 + i // RADIUS, 1),
                :,
                pl.ds(RADIUS + depth + i % RADIUS, 1),
                pl.ds(PAD, height),
                :,
            ] = zero_plane
            return carry

        lax.fori_loop(0, STEPS * RADIUS, clear, 0)

    for copy in small:
        copy.wait()
    source = [source_ref[0, i] for i in range(3)]
    levels = index.shape[0]
    flat_index = index[...].reshape(levels * depth, index.shape[2])

    def look_up(k, acc):
        return jnp.where(flat_index == k, table[k], acc)

    looked = lax.fori_loop(0, table.shape[0], look_up, jnp.zeros(flat_index.shape, jnp.float32))
    scales[pl.ds(0, levels * depth), :] = looked
    scales[pl.ds(levels * depth, LANES - levels * depth), :] = jnp.zeros(
        (LANES - levels * depth, index.shape[2]), jnp.float32
    )
    flipped[...] = scales[...].T
    width = 4 * LANES
    cell = cells[...] - me * (depth * height * width)
    row_of = cell // width
    col_of = cell % width
    block_of = (cell // LANES) % (4 * height)
    slab_of = row_of // height
    for z in range(depth):
        ids = z * height + lax.broadcasted_iota(jnp.int32, (height, receivers), 0)
        rows_hot[z] = jnp.where(ids == row_of, 1.0, 0.0).astype(jnp.bfloat16)
    col_ids = lax.broadcasted_iota(jnp.int32, (width, receivers), 0)
    cols_hot[...] = jnp.where(col_ids == col_of, 1.0, 0.0).astype(jnp.bfloat16)
    block_ids = lax.broadcasted_iota(jnp.int32, (4 * height, receivers), 0)
    blocks_hot = jnp.where(block_ids == block_of, 1.0, 0.0)
    scale_at = jnp.dot(
        scales[...], blocks_hot, precision=lax.Precision.HIGHEST, preferred_element_type=jnp.float32
    )
    depth_ids = lax.broadcasted_iota(jnp.int32, (depth, receivers), 0)
    small_words.wait()
    planes = 4
    total = jnp.zeros((1, receivers), jnp.float32)
    for t in range(STEPS):
        level = STEPS - t

        def gather(i, acc):
            w = words[level, pl.ds(i * planes, planes), :, :].reshape(planes * height, LANES)
            parts = [
                (((w >> (8 * m)) & 255) - 128).astype(jnp.float32).astype(jnp.bfloat16)
                for m in range(4)
            ]
            found = jnp.dot(
                jnp.concatenate(parts, axis=1), cols_hot[...], preferred_element_type=jnp.float32
            )
            hot = rows_hot[pl.ds(i * planes, planes), :, :].reshape(planes * height, receivers)
            return acc + jnp.sum(found * hot.astype(jnp.float32), axis=0, keepdims=True)

        code = lax.fori_loop(
            0, depth // planes, gather, jnp.zeros((1, receivers), jnp.float32)
        )
        part = scale_at[level * depth : (level + 1) * depth]
        factor = jnp.sum(jnp.where(depth_ids == slab_of, part, 0.0), axis=0, keepdims=True)
        residual = code * factor - observed[level - 1 : level, :]
        total = total + residual * residual
        left = residual
        for piece in range(3):
            short = left.astype(jnp.bfloat16).astype(jnp.float32)
            left = left - short
            values[t, piece] = jnp.where(col_ids == col_of, short, 0.0).astype(jnp.bfloat16)
    sums[0] = jnp.broadcast_to(
        jnp.sum(total, axis=1, keepdims=True), sums.shape[1:]
    )

    def sum_copy(b):
        return pltpu.make_async_remote_copy(
            src_ref=sums.at[b],
            dst_ref=sums_in.at[b],
            send_sem=sum_send.at[b],
            recv_sem=sum_recv.at[b],
            device_id=stages[b],
            device_id_type=MESH,
        )

    for copy in rest:
        copy.wait()

    lane = lax.broadcasted_iota(jnp.int32, (tall, LANES), 1)

    def update(t, c, row, z):
        def at(xc, dz, dy):
            return field[1 + t, xc, RADIUS + z + dz, pl.ds(row + dy, tall), :]

        centre = [at(xc, 0, 0) for xc in range(4)]
        after = [[pltpu.roll(v, LANES - i, 1) for v in centre] for i in range(1, 5)]
        before = [[pltpu.roll(v, i, 1) for v in centre] for i in range(1, 5)]
        for xc in range(4):
            acc = (3.0 * COEFFS[0]) * centre[xc]
            for i in range(1, 5):
                nxt = after[i - 1][xc + 1] if xc < 3 else 0.0
                prv = before[i - 1][xc - 1] if xc > 0 else 0.0
                pair = jnp.where(lane < LANES - i, after[i - 1][xc], nxt) + jnp.where(
                    lane >= i, before[i - 1][xc], prv
                )
                pair = pair + (at(xc, i, 0) + at(xc, -i, 0)) + (at(xc, 0, i) + at(xc, 0, -i))
                acc = acc + COEFFS[i] * pair
            y0 = pl.multiple_of(row - PAD, 8)
            old = field[t, xc, RADIUS + z, pl.ds(row, tall), :]
            new = 2.0 * centre[xc] - old + courant[xc, z, pl.ds(y0, tall), :] * acc
            field[(2 + t) % (STEPS + 1), xc, RADIUS + z, pl.ds(row, tall), :] = (
                new + injected[xc, z, :, :]
            )

    def inject(t, c):
        hot = rows_hot[:, pl.ds(pl.multiple_of(c * tall, 16), tall), :].reshape(
            depth * tall, receivers
        )
        acc = None
        for piece in range(3):
            term = lax.dot_general(
                hot,
                values[t, piece],
                (((1,), (1,)), ((), ())),
                preferred_element_type=jnp.float32,
            )
            acc = term if acc is None else acc + term
        for xc in range(4):
            injected[xc] = acc[:, xc * LANES : (xc + 1) * LANES].reshape(depth, tall, LANES)

    def spread_rows(c):
        row = pl.multiple_of(c * tall, 8)
        columns = [
            flipped[pl.ds(pl.multiple_of(4 * c * tall, 8) + m, tall, stride=4), :]
            for m in range(4)
        ]
        for i in range(levels * depth):
            for m in range(4):
                spread[i // depth, i % depth, m, pl.ds(row, tall), :] = jnp.broadcast_to(
                    columns[m][:, i : i + 1], (tall, LANES)
                )

    def add_image(t, c, row, first):
        level = STEPS - t
        y0 = pl.multiple_of(row - PAD, 8)

        def plane(z, carry):
            ws = [words[level + d, z, pl.ds(y0, tall), :] for d in (-1, 0, 1)]
            for m in range(4):
                f = [
                    (((w >> (8 * m)) & 255) - 128).astype(jnp.float32)
                    * spread[level + d, z, m, pl.ds(y0, tall), :]
                    for w, d in zip(ws, (-1, 0, 1))
                ]
                term = field[1 + t, m, RADIUS + z, pl.ds(row, tall), :] * (
                    f[2] - 2.0 * f[1] + f[0]
                )
                if first:
                    image[c, m, z] = term
                else:
                    image[c, m, z] = image[c, m, z] + term
            return carry

        lax.fori_loop(0, depth, plane, 0)

    def mute(c):
        y = c * tall + lax.broadcasted_iota(jnp.int32, (tall, LANES), 0)
        across = [(y - source[1]) ** 2 + (m * LANES + lane - source[2]) ** 2 for m in range(4)]

        def plane(z, carry):
            dz = me * depth + z - source[0]
            for m in range(4):
                dist = (across[m] + dz * dz).astype(jnp.float32)
                image[c, m, z] = image[c, m, z] * (1.0 - jnp.exp(-dist / (2.0 * MUTE * MUTE)))
            return carry

        lax.fori_loop(0, depth, plane, 0)

    far = 2 * (1 - side) + core
    near = shot

    def pair_copy(c, slot):
        return pltpu.make_async_remote_copy(
            src_ref=image.at[c],
            dst_ref=from_sibling.at[slot],
            send_sem=image_send.at[slot],
            recv_sem=image_recv.at[slot],
            device_id={"shot": sibling},
            device_id_type=MESH,
        )

    sibling_far = 2 * (1 - side) + 1 - core
    far_copy = pair_copy(sibling_far, 0)
    near_copy = pair_copy(sibling, 1)
    partner_copy = pltpu.make_async_remote_copy(
        src_ref=combined,
        dst_ref=from_partner,
        send_sem=image_send.at[2],
        recv_sem=image_recv.at[2],
        device_id={"shot": partner},
        device_id_type=MESH,
    )

    outs = []

    def store(src, dst):
        copy = pltpu.make_async_copy(src, dst, out_sem.at[len(outs)])
        copy.start()
        outs.append(copy)

    def first_copy(n, xc):
        c, row = rows_of(n)
        return pltpu.make_async_copy(
            field.at[0, xc, pl.ds(RADIUS, depth), pl.ds(row, tall), :],
            first_hbm.at[0, :, pl.ds(pl.multiple_of(row - PAD, 8), tall), lanes(xc)],
            out_sem.at[16 + n * 4 + xc],
        )

    for t in range(STEPS):

        def task(n, carry, t=t):
            c, row = rows_of(n)
            if t < 2:
                for j in range(4):
                    b = 4 * t + j

                    @pl.when(n == j)
                    def _():
                        if b > 0:
                            sum_copy(b - 1).wait_recv()
                            sums[b] = sums[b - 1] + sums_in[b - 1]
                        sum_copy(b).start()

            inject(t, c)

            def inner(z, carry):
                update(t, c, row, z)
                return carry

            lax.fori_loop(RADIUS, depth - RADIUS, inner, 0)
            if t == 0:
                spread_rows(c)
                add_image(0, c, row, True)
            if t == 2:

                @pl.when(n == 2)
                def _():
                    far_copy.wait_recv()

                    def plane(z, carry):
                        for m in range(4):
                            combined[m, z] = image[far, m, z] + from_sibling[0, m, z]
                        return carry

                    lax.fori_loop(0, depth, plane, 0)
                    partner_copy.start()

            if t == 3:

                @pl.when(n == 3)
                def _():
                    near_copy.wait_recv()
                    partner_copy.wait_recv()

                    def plane(z, carry):
                        for m in range(4):
                            grad_out[m, z] = (
                                image[near, m, z] + from_sibling[1, m, z] + from_partner[m, z]
                            )
                        return carry

                    lax.fori_loop(0, depth, plane, 0)

            @pl.when(has_down)
            def _():
                halo_copy(t, n, 0).wait_recv()

            lax.fori_loop(0, RADIUS, inner, 0)
            if t < STEPS - 1:

                @pl.when(has_down)
                def _():
                    halo_copy(t + 1, n, 1).start()

            @pl.when(has_up)
            def _():
                halo_copy(t, n, 1).wait_recv()

            lax.fori_loop(depth - RADIUS, depth, inner, 0)
            if t < STEPS - 1:

                @pl.when(has_up)
                def _():
                    halo_copy(t + 1, n, 0).start()

                add_image(t + 1, c, row, False)
            else:
                for xc in range(4):
                    first_copy(n, xc).start()
            if t == 2:
                mute(c)

                @pl.when(c == sibling_far)
                def _():
                    far_copy.start()

                @pl.when(c == sibling)
                def _():
                    near_copy.start()

            return carry

        lax.fori_loop(0, CHUNKS, task, 0)
        if t == 1:
            last = len(stages) - 1
            sum_copy(last).wait_recv()
            sums[last + 1] = (sums[last] + sums_in[last]) * scale
        if t == 2:
            for xc in range(4):
                store(
                    field.at[STEPS, xc, pl.ds(RADIUS, depth), pl.ds(PAD, height), :],
                    second_hbm.at[0, :, :, lanes(xc)],
                )
            store(sums.at[len(stages)], misfit_hbm)
    for xc in range(4):
        store(grad_out.at[xc], grad_hbm.at[:, :, lanes(xc)])

    def drain(n, carry):
        for t in range(STEPS):

            @pl.when(has_up)
            def _():
                halo_copy(t, n, 0).wait_send()

            @pl.when(has_down)
            def _():
                halo_copy(t, n, 1).wait_send()

        for xc in range(4):
            first_copy(n, xc).wait()
        return carry

    far_copy.wait_send()
    near_copy.wait_send()
    partner_copy.wait_send()
    for b in range(len(stages)):
        sum_copy(b).wait_send()
    lax.fori_loop(0, CHUNKS, drain, 0)
    for copy in outs:
        copy.wait()


def finish(g_in, f_in, s_in, m_in, g_out, f_out, s_out, m_out, tile, one, sem):
    pairs = [(m_in, tile), (f_in, f_out), (s_in, s_out), (g_in, g_out)]
    copies = [pltpu.make_async_copy(a, b, sem.at[i]) for i, (a, b) in enumerate(pairs)]
    for copy in copies:
        copy.start()
    copies[0].wait()
    one[...] = tile[0:1, 0:1]
    last = pltpu.make_async_copy(one, m_out, sem.at[len(pairs)])
    last.start()
    for copy in copies[1:]:
        copy.wait()
    last.wait()


def body(
    space_size,
    shot_size,
    adjoint_now,
    adjoint_later,
    courant,
    checkpoint_codes,
    scale_index,
    scale_table,
    receiver_cell,
    observed,
    source_cell,
):
    _, depth, height, width = adjoint_now.shape
    levels = checkpoint_codes.shape[1]
    receivers = receiver_cell.shape[1]
    tall = height // CHUNKS
    quarter = (4, depth, tall, LANES)
    stages = (space_size * shot_size).bit_length() - 1
    whole = pl.BlockSpec(memory_space=pl.ANY)
    outside = pl.BlockSpec(memory_space=pltpu.HBM)
    f32 = jnp.float32
    results = pl.pallas_call(
        functools.partial(kernel, space_size, shot_size),
        out_shape=(
            jax.ShapeDtypeStruct((depth, tall, width), f32),
            jax.ShapeDtypeStruct(adjoint_now.shape, f32),
            jax.ShapeDtypeStruct(adjoint_now.shape, f32),
            jax.ShapeDtypeStruct((8, LANES), f32),
        ),
        in_specs=[outside] * 9,
        out_specs=[whole] * 4,
        scratch_shapes=[
            pltpu.SMEM(scale_table.shape, f32),
            pltpu.SMEM(source_cell.shape, jnp.int32),
            pltpu.VMEM((STEPS + 1, 4, depth + 2 * RADIUS, height + 2 * PAD, LANES), f32),
            pltpu.VMEM((4, depth, height, LANES), f32),
            pltpu.VMEM((levels, depth, height, LANES), jnp.int32),
            pltpu.VMEM((levels, depth, 4 * height), jnp.int32),
            pltpu.VMEM((1, receivers), jnp.int32),
            pltpu.VMEM((STEPS, receivers), f32),
            pltpu.VMEM((LANES, 4 * height), f32),
            pltpu.VMEM((4 * height, LANES), f32),
            pltpu.VMEM((levels, depth, 4, height, LANES), f32),
            pltpu.VMEM((depth, height, receivers), jnp.bfloat16),
            pltpu.VMEM((width, receivers), jnp.bfloat16),
            pltpu.VMEM((STEPS, 3, width, receivers), jnp.bfloat16),
            pltpu.VMEM(quarter, f32),
            pltpu.VMEM((CHUNKS, *quarter), f32),
            pltpu.VMEM((2, *quarter), f32),
            pltpu.VMEM(quarter, f32),
            pltpu.VMEM(quarter, f32),
            pltpu.VMEM(quarter, f32),
            pltpu.VMEM((stages + 1, 8, LANES), f32),
            pltpu.VMEM((stages, 8, LANES), f32),
            pltpu.SemaphoreType.DMA((32,)),
            pltpu.SemaphoreType.DMA((32,)),
            pltpu.SemaphoreType.DMA((2, STEPS, CHUNKS)),
            pltpu.SemaphoreType.DMA((2, STEPS, CHUNKS)),
            pltpu.SemaphoreType.DMA((3,)),
            pltpu.SemaphoreType.DMA((3,)),
            pltpu.SemaphoreType.DMA((stages,)),
            pltpu.SemaphoreType.DMA((stages,)),
        ],
        compiler_params=pltpu.CompilerParams(
            collective_id=0, has_side_effects=True, vmem_limit_bytes=48 * 1024 * 1024
        ),
    )(
        *(
            pltpu.with_memory_space_constraint(x, pltpu.HBM)
            for x in (
                adjoint_now,
                adjoint_later,
                courant,
                checkpoint_codes,
                scale_index,
                receiver_cell,
                observed,
                scale_table,
                source_cell,
            )
        )
    )
    gradient, first, second, misfit = pl.pallas_call(
        finish,
        out_shape=tuple(
            jax.ShapeDtypeStruct(x.shape if i < 3 else (1, 1), f32) for i, x in enumerate(results)
        ),
        in_specs=[whole] * 4,
        out_specs=[outside] * 4,
        scratch_shapes=[
            pltpu.VMEM((8, LANES), f32),
            pltpu.VMEM((1, 1), f32),
            pltpu.SemaphoreType.DMA((5,)),
        ],
        compiler_params=pltpu.CompilerParams(vmem_limit_bytes=1024 * 1024),
    )(*results)
    return gradient, first, second, misfit.reshape(())


def solution(mesh):
    sizes = dict(mesh.shape)
    return jax.shard_map(
        functools.partial(body, sizes["space"], sizes["shot"]),
        mesh=mesh,
        in_specs=(
            P("shot", "space", None, None),
            P("shot", "space", None, None),
            P("space", None, None),
            P("shot", None, "space", None, None),
            P("shot", None, "space", None),
            P(),
            P("shot", "space"),
            P("shot", None, "space"),
            P("shot", None),
        ),
        out_specs=(
            P("space", "shot", None),
            P("shot", "space", None, None),
            P("shot", "space", None, None),
            P(),
        ),
        check_vma=False,
    )
```

```python
import functools

import jax
import jax.numpy as jnp
from jax import lax
from jax.experimental import pallas as pl
from jax.experimental.pallas import tpu as pltpu
from jax.sharding import PartitionSpec as P

STEPS = 4
MUTE = 8
RADIUS = 4
LANES = 128
PAD = 8
CHUNKS = 4
COEFFS = (-205.0 / 72.0, 8.0 / 5.0, -1.0 / 5.0, 8.0 / 315.0, -1.0 / 560.0)
MESH = pl.DeviceIdType.MESH


def kernel(
    space_size,
    shot_size,
    now_hbm,
    later_hbm,
    courant_hbm,
    codes_hbm,
    index_hbm,
    cells_hbm,
    observed_hbm,
    table_hbm,
    source_hbm,
    grad_hbm,
    first_hbm,
    second_hbm,
    misfit_hbm,
    table,
    source_ref,
    field,
    courant,
    words,
    index,
    cells,
    observed,
    scales,
    flipped,
    spread,
    rows_hot,
    cols_hot,
    values,
    injected,
    scale_at,
    image,
    from_sibling,
    combined,
    from_partner,
    grad_out,
    sums,
    sums_in,
    load_sem,
    out_sem,
    halo_send,
    halo_recv,
    image_send,
    image_recv,
    sum_send,
    sum_recv,
):
    scale = 0.5 / (shot_size * STEPS * cells.shape[1] * space_size)
    depth = courant.shape[1]
    height = courant.shape[2]
    tall = height // CHUNKS
    receivers = cells.shape[1]
    me = lax.axis_index("space")
    shot = lax.axis_index("shot")
    side, core = shot // 2, shot % 2
    up, down = (me + 1) % space_size, (me + space_size - 1) % space_size
    sibling = shot + 1 - 2 * core
    partner = (shot + 2) % 4

    def flip(i, bit):
        return i + bit - 2 * bit * ((i // bit) % 2)

    stages = []
    bit = 1
    while bit < space_size:
        stages.append({"space": flip(me, bit)})
        bit *= 2
    bit = 1
    while bit < shot_size:
        stages.append({"shot": flip(shot, bit)})
        bit *= 2
    peers = stages + [{"space": up}, {"space": down}]
    barrier = pltpu.get_barrier_semaphore()
    for peer in peers:
        pl.semaphore_signal(barrier, inc=1, device_id=peer, device_id_type=MESH)

    loads = []

    def load(src, dst):
        copy = pltpu.make_async_copy(src, dst, load_sem.at[len(loads)])
        copy.start()
        loads.append(copy)
        return copy

    def lanes(xc):
        return pl.ds(xc * LANES, LANES)

    edges = []
    for xc in range(4):
        for z in (0, depth - RADIUS):
            edges.append(
                load(
                    now_hbm.at[0, pl.ds(z, RADIUS), :, lanes(xc)],
                    field.at[1, xc, pl.ds(RADIUS + z, RADIUS), pl.ds(PAD, height), :],
                )
            )
    small = [
        load(index_hbm.at[0], index),
        load(cells_hbm, cells),
        load(observed_hbm.at[0], observed),
        load(table_hbm, table),
        load(source_hbm, source_ref),
    ]
    small_words = load(codes_hbm.at[0], words)
    rest = []
    for xc in range(4):
        rest.append(
            load(
                now_hbm.at[0, pl.ds(RADIUS, depth - 2 * RADIUS), :, lanes(xc)],
                field.at[1, xc, pl.ds(2 * RADIUS, depth - 2 * RADIUS), pl.ds(PAD, height), :],
            )
        )
        rest.append(
            load(
                later_hbm.at[0, :, :, lanes(xc)],
                field.at[0, xc, pl.ds(RADIUS, depth), pl.ds(PAD, height), :],
            )
        )
        rest.append(load(courant_hbm.at[:, :, lanes(xc)], courant.at[xc]))

    pl.semaphore_wait(barrier, len(peers))

    def rows_of(n):
        c = (n + 2 * (1 - side)) % CHUNKS
        return c, pl.multiple_of(PAD + c * tall, 8)

    def halo_copy(t, n, way):
        _, row = rows_of(n)
        src_z, dst_z, target = ((depth, 0, up), (RADIUS, RADIUS + depth, down))[way]
        return pltpu.make_async_remote_copy(
            src_ref=field.at[1 + t, :, pl.ds(src_z, RADIUS), pl.ds(row, tall), :],
            dst_ref=field.at[1 + t, :, pl.ds(dst_z, RADIUS), pl.ds(row, tall), :],
            send_sem=halo_send.at[way, t, n],
            recv_sem=halo_recv.at[way, t, n],
            device_id={"space": target},
            device_id_type=MESH,
        )

    has_up = me < space_size - 1
    has_down = me > 0

    def send_halo(t, n):
        @pl.when(has_up)
        def _():
            halo_copy(t, n, 0).start()

        @pl.when(has_down)
        def _():
            halo_copy(t, n, 1).start()

    for copy in edges:
        copy.wait()

    def first_sends(n, carry):
        send_halo(0, n)
        return carry

    lax.fori_loop(0, CHUNKS, first_sends, 0)

    zero_rows = jnp.zeros((4, 1, PAD, LANES), jnp.float32)

    def clear_rows(i, carry):
        level = 1 + i // depth
        z = RADIUS + i % depth
        field[pl.ds(level, 1), :, pl.ds(z, 1), pl.ds(0, PAD), :] = zero_rows[None]
        field[pl.ds(level, 1), :, pl.ds(z, 1), pl.ds(PAD + height, PAD), :] = zero_rows[None]
        return carry

    lax.fori_loop(0, STEPS * depth, clear_rows, 0)
    zero_plane = jnp.zeros((1, 4, 1, height, LANES), jnp.float32)

    @pl.when(me == 0)
    def _():
        def clear(i, carry):
            field[pl.ds(1 + i // RADIUS, 1), :, pl.ds(i % RADIUS, 1), pl.ds(PAD, height), :] = (
                zero_plane
            )
            return carry

        lax.fori_loop(0, STEPS * RADIUS, clear, 0)

    @pl.when(me == space_size - 1)
    def _():
        def clear(i, carry):
            field[
                pl.ds(1 + i // RADIUS, 1),
                :,
                pl.ds(RADIUS + depth + i % RADIUS, 1),
                pl.ds(PAD, height),
                :,
            ] = zero_plane
            return carry

        lax.fori_loop(0, STEPS * RADIUS, clear, 0)

    for copy in small:
        copy.wait()
    source = [source_ref[0, i] for i in range(3)]
    levels = index.shape[0]
    flat_index = index[...].reshape(levels * depth, index.shape[2])

    def look_up(k, acc):
        return jnp.where(flat_index == k, table[k], acc)

    looked = lax.fori_loop(0, table.shape[0], look_up, jnp.zeros(flat_index.shape, jnp.float32))
    scales[pl.ds(0, levels * depth), :] = looked
    scales[pl.ds(levels * depth, LANES - levels * depth), :] = jnp.zeros(
        (LANES - levels * depth, index.shape[2]), jnp.float32
    )
    flipped[...] = scales[...].T
    width = 4 * LANES
    cell = cells[...] - me * (depth * height * width)
    row_of = cell // width
    col_of = cell % width
    block_of = (cell // LANES) % (4 * height)
    slab_of = row_of // height
    for z in range(depth):
        ids = z * height + lax.broadcasted_iota(jnp.int32, (height, receivers), 0)
        rows_hot[z] = jnp.where(ids == row_of, 1.0, 0.0).astype(jnp.bfloat16)
    col_ids = lax.broadcasted_iota(jnp.int32, (width, receivers), 0)
    cols_hot[...] = jnp.where(col_ids == col_of, 1.0, 0.0).astype(jnp.bfloat16)
    block_ids = lax.broadcasted_iota(jnp.int32, (4 * height, receivers), 0)
    blocks_hot = jnp.where(block_ids == block_of, 1.0, 0.0)
    scale_at[...] = jnp.dot(
        scales[...], blocks_hot, precision=lax.Precision.HIGHEST, preferred_element_type=jnp.float32
    )
    depth_ids = lax.broadcasted_iota(jnp.int32, (depth, receivers), 0)
    small_words.wait()
    planes = 4

    def residuals(t):
        level = STEPS - t

        def gather(i, acc):
            w = words[level, pl.ds(i * planes, planes), :, :].reshape(planes * height, LANES)
            parts = [
                (((w >> (8 * m)) & 255) - 128).astype(jnp.float32).astype(jnp.bfloat16)
                for m in range(4)
            ]
            found = jnp.dot(
                jnp.concatenate(parts, axis=1), cols_hot[...], preferred_element_type=jnp.float32
            )
            hot = rows_hot[pl.ds(i * planes, planes), :, :].reshape(planes * height, receivers)
            return acc + jnp.sum(found * hot.astype(jnp.float32), axis=0, keepdims=True)

        code = lax.fori_loop(0, depth // planes, gather, jnp.zeros((1, receivers), jnp.float32))
        part = scale_at[pl.ds(level * depth, depth), :]
        factor = jnp.sum(jnp.where(depth_ids == slab_of, part, 0.0), axis=0, keepdims=True)
        residual = code * factor - observed[level - 1 : level, :]
        squares = jnp.broadcast_to(
            jnp.sum(residual * residual, axis=1, keepdims=True), sums.shape[1:]
        )
        sums[0] = squares if t == 0 else sums[0] + squares
        left = residual
        for piece in range(3):
            short = left.astype(jnp.bfloat16).astype(jnp.float32)
            left = left - short
            values[t, piece] = jnp.where(col_ids == col_of, short, 0.0).astype(jnp.bfloat16)

    residuals(0)

    def sum_copy(b):
        return pltpu.make_async_remote_copy(
            src_ref=sums.at[b],
            dst_ref=sums_in.at[b],
            send_sem=sum_send.at[b],
            recv_sem=sum_recv.at[b],
            device_id=stages[b],
            device_id_type=MESH,
        )

    for copy in rest:
        copy.wait()

    lane = lax.broadcasted_iota(jnp.int32, (tall, LANES), 1)

    def update(t, c, row, z):
        def at(xc, dz, dy):
            return field[1 + t, xc, RADIUS + z + dz, pl.ds(row + dy, tall), :]

        centre = [at(xc, 0, 0) for xc in range(4)]
        after = [[pltpu.roll(v, LANES - i, 1) for v in centre] for i in range(1, 5)]
        before = [[pltpu.roll(v, i, 1) for v in centre] for i in range(1, 5)]
        for xc in range(4):
            acc = (3.0 * COEFFS[0]) * centre[xc]
            for i in range(1, 5):
                nxt = after[i - 1][xc + 1] if xc < 3 else 0.0
                prv = before[i - 1][xc - 1] if xc > 0 else 0.0
                pair = jnp.where(lane < LANES - i, after[i - 1][xc], nxt) + jnp.where(
                    lane >= i, before[i - 1][xc], prv
                )
                pair = pair + (at(xc, i, 0) + at(xc, -i, 0)) + (at(xc, 0, i) + at(xc, 0, -i))
                acc = acc + COEFFS[i] * pair
            y0 = pl.multiple_of(row - PAD, 8)
            old = field[t, xc, RADIUS + z, pl.ds(row, tall), :]
            new = 2.0 * centre[xc] - old + courant[xc, z, pl.ds(y0, tall), :] * acc
            field[(2 + t) % (STEPS + 1), xc, RADIUS + z, pl.ds(row, tall), :] = (
                new + injected[xc, z, :, :]
            )

    def inject(t, c):
        hot = rows_hot[:, pl.ds(pl.multiple_of(c * tall, 16), tall), :].reshape(
            depth * tall, receivers
        )
        acc = None
        for piece in range(3):
            term = lax.dot_general(
                hot,
                values[t, piece],
                (((1,), (1,)), ((), ())),
                preferred_element_type=jnp.float32,
            )
            acc = term if acc is None else acc + term
        for xc in range(4):
            injected[xc] = acc[:, xc * LANES : (xc + 1) * LANES].reshape(depth, tall, LANES)

    def spread_rows(c):
        row = pl.multiple_of(c * tall, 8)
        columns = [
            flipped[pl.ds(pl.multiple_of(4 * c * tall, 8) + m, tall, stride=4), :]
            for m in range(4)
        ]
        for i in range(levels * depth):
            for m in range(4):
                spread[i // depth, i % depth, m, pl.ds(row, tall), :] = jnp.broadcast_to(
                    columns[m][:, i : i + 1], (tall, LANES)
                )

    def add_image(t, c, row, first):
        level = STEPS - t
        y0 = pl.multiple_of(row - PAD, 8)

        def plane(z, carry):
            ws = [words[level + d, z, pl.ds(y0, tall), :] for d in (-1, 0, 1)]
            for m in range(4):
                f = [
                    (((w >> (8 * m)) & 255) - 128).astype(jnp.float32)
                    * spread[level + d, z, m, pl.ds(y0, tall), :]
                    for w, d in zip(ws, (-1, 0, 1))
                ]
                term = field[1 + t, m, RADIUS + z, pl.ds(row, tall), :] * (
                    f[2] - 2.0 * f[1] + f[0]
                )
                if first:
                    image[c, m, z] = term
                else:
                    image[c, m, z] = image[c, m, z] + term
            return carry

        lax.fori_loop(0, depth, plane, 0)

    def mute(c):
        y = c * tall + lax.broadcasted_iota(jnp.int32, (tall, LANES), 0)
        across = [(y - source[1]) ** 2 + (m * LANES + lane - source[2]) ** 2 for m in range(4)]

        def plane(z, carry):
            dz = me * depth + z - source[0]
            for m in range(4):
                dist = (across[m] + dz * dz).astype(jnp.float32)
                image[c, m, z] = image[c, m, z] * (1.0 - jnp.exp(-dist / (2.0 * MUTE * MUTE)))
            return carry

        lax.fori_loop(0, depth, plane, 0)

    far = 2 * (1 - side) + core
    near = shot

    def pair_copy(c, slot):
        return pltpu.make_async_remote_copy(
            src_ref=image.at[c],
            dst_ref=from_sibling.at[slot],
            send_sem=image_send.at[slot],
            recv_sem=image_recv.at[slot],
            device_id={"shot": sibling},
            device_id_type=MESH,
        )

    sibling_far = 2 * (1 - side) + 1 - core
    far_copy = pair_copy(sibling_far, 0)
    near_copy = pair_copy(sibling, 1)
    partner_copy = pltpu.make_async_remote_copy(
        src_ref=combined,
        dst_ref=from_partner,
        send_sem=image_send.at[2],
        recv_sem=image_recv.at[2],
        device_id={"shot": partner},
        device_id_type=MESH,
    )

    outs = []

    def store(src, dst):
        copy = pltpu.make_async_copy(src, dst, out_sem.at[len(outs)])
        copy.start()
        outs.append(copy)

    def first_copy(n, xc):
        c, row = rows_of(n)
        return pltpu.make_async_copy(
            field.at[0, xc, pl.ds(RADIUS, depth), pl.ds(row, tall), :],
            first_hbm.at[0, :, pl.ds(pl.multiple_of(row - PAD, 8), tall), lanes(xc)],
            out_sem.at[16 + n * 4 + xc],
        )

    for t in range(STEPS):

        def task(n, carry, t=t):
            c, row = rows_of(n)
            if t in (1, 2):
                for j in range(4):
                    b = 4 * (t - 1) + j

                    @pl.when(n == j)
                    def _():
                        if b > 0:
                            sum_copy(b - 1).wait_recv()
                            sums[b] = sums[b - 1] + sums_in[b - 1]
                        sum_copy(b).start()

            inject(t, c)

            def inner(z, carry):
                update(t, c, row, z)
                return carry

            lax.fori_loop(RADIUS, depth - RADIUS, inner, 0)
            if t == 3:

                @pl.when(n == 0)
                def _():
                    far_copy.wait_recv()

                    def plane(z, carry):
                        for m in range(4):
                            combined[m, z] = image[far, m, z] + from_sibling[0, m, z]
                        return carry

                    lax.fori_loop(0, depth, plane, 0)
                    partner_copy.start()

            @pl.when(has_down)
            def _():
                halo_copy(t, n, 0).wait_recv()

            lax.fori_loop(0, RADIUS, inner, 0)
            if t < STEPS - 1:

                @pl.when(has_down)
                def _():
                    halo_copy(t + 1, n, 1).start()

            @pl.when(has_up)
            def _():
                halo_copy(t, n, 1).wait_recv()

            lax.fori_loop(depth - RADIUS, depth, inner, 0)
            if t < STEPS - 1:

                @pl.when(has_up)
                def _():
                    halo_copy(t + 1, n, 0).start()

            if t == 0:
                for j in range(1, STEPS):

                    @pl.when(n == j - 1)
                    def _():
                        residuals(j)

            if t == 1:
                spread_rows(c)
                add_image(0, c, row, True)
                add_image(1, c, row, False)
            if t == 2:
                add_image(2, c, row, False)
                add_image(3, c, row, False)
            if t == STEPS - 1:
                for xc in range(4):
                    first_copy(n, xc).start()
            if t == 2:
                mute(c)

                @pl.when(c == sibling_far)
                def _():
                    far_copy.start()

                @pl.when(c == sibling)
                def _():
                    near_copy.start()

            return carry

        lax.fori_loop(0, CHUNKS, task, 0)
        if t == 2:
            last = len(stages) - 1
            sum_copy(last).wait_recv()
            sums[last + 1] = (sums[last] + sums_in[last]) * scale
        if t == 2:
            for xc in range(4):
                store(
                    field.at[STEPS, xc, pl.ds(RADIUS, depth), pl.ds(PAD, height), :],
                    second_hbm.at[0, :, :, lanes(xc)],
                )
            store(sums.at[len(stages)], misfit_hbm)
    near_copy.wait_recv()
    partner_copy.wait_recv()

    def plane(z, carry):
        for m in range(4):
            grad_out[m, z] = (
                image[near, m, z] + from_sibling[1, m, z] + from_partner[m, z]
            )
        return carry

    lax.fori_loop(0, depth, plane, 0)
    for xc in range(4):
        store(grad_out.at[xc], grad_hbm.at[:, :, lanes(xc)])

    def drain(n, carry):
        for t in range(STEPS):

            @pl.when(has_up)
            def _():
                halo_copy(t, n, 0).wait_send()

            @pl.when(has_down)
            def _():
                halo_copy(t, n, 1).wait_send()

        for xc in range(4):
            first_copy(n, xc).wait()
        return carry

    far_copy.wait_send()
    near_copy.wait_send()
    partner_copy.wait_send()
    for b in range(len(stages)):
        sum_copy(b).wait_send()
    lax.fori_loop(0, CHUNKS, drain, 0)
    for copy in outs:
        copy.wait()


def finish(g_in, f_in, s_in, m_in, g_out, f_out, s_out, m_out, tile, one, sem):
    pairs = [(m_in, tile), (f_in, f_out), (s_in, s_out), (g_in, g_out)]
    copies = [pltpu.make_async_copy(a, b, sem.at[i]) for i, (a, b) in enumerate(pairs)]
    for copy in copies:
        copy.start()
    copies[0].wait()
    one[...] = tile[0:1, 0:1]
    last = pltpu.make_async_copy(one, m_out, sem.at[len(pairs)])
    last.start()
    for copy in copies[1:]:
        copy.wait()
    last.wait()


def body(
    space_size,
    shot_size,
    adjoint_now,
    adjoint_later,
    courant,
    checkpoint_codes,
    scale_index,
    scale_table,
    receiver_cell,
    observed,
    source_cell,
):
    _, depth, height, width = adjoint_now.shape
    levels = checkpoint_codes.shape[1]
    receivers = receiver_cell.shape[1]
    tall = height // CHUNKS
    quarter = (4, depth, tall, LANES)
    stages = (space_size * shot_size).bit_length() - 1
    whole = pl.BlockSpec(memory_space=pl.ANY)
    outside = pl.BlockSpec(memory_space=pltpu.HBM)
    f32 = jnp.float32
    results = pl.pallas_call(
        functools.partial(kernel, space_size, shot_size),
        out_shape=(
            jax.ShapeDtypeStruct((depth, tall, width), f32),
            jax.ShapeDtypeStruct(adjoint_now.shape, f32),
            jax.ShapeDtypeStruct(adjoint_now.shape, f32),
            jax.ShapeDtypeStruct((8, LANES), f32),
        ),
        in_specs=[outside] * 9,
        out_specs=[whole] * 4,
        scratch_shapes=[
            pltpu.SMEM(scale_table.shape, f32),
            pltpu.SMEM(source_cell.shape, jnp.int32),
            pltpu.VMEM((STEPS + 1, 4, depth + 2 * RADIUS, height + 2 * PAD, LANES), f32),
            pltpu.VMEM((4, depth, height, LANES), f32),
            pltpu.VMEM((levels, depth, height, LANES), jnp.int32),
            pltpu.VMEM((levels, depth, 4 * height), jnp.int32),
            pltpu.VMEM((1, receivers), jnp.int32),
            pltpu.VMEM((STEPS, receivers), f32),
            pltpu.VMEM((LANES, 4 * height), f32),
            pltpu.VMEM((4 * height, LANES), f32),
            pltpu.VMEM((levels, depth, 4, height, LANES), f32),
            pltpu.VMEM((depth, height, receivers), jnp.bfloat16),
            pltpu.VMEM((width, receivers), jnp.bfloat16),
            pltpu.VMEM((STEPS, 3, width, receivers), jnp.bfloat16),
            pltpu.VMEM(quarter, f32),
            pltpu.VMEM((LANES, receivers), f32),
            pltpu.VMEM((CHUNKS, *quarter), f32),
            pltpu.VMEM((2, *quarter), f32),
            pltpu.VMEM(quarter, f32),
            pltpu.VMEM(quarter, f32),
            pltpu.VMEM(quarter, f32),
            pltpu.VMEM((stages + 1, 8, LANES), f32),
            pltpu.VMEM((stages, 8, LANES), f32),
            pltpu.SemaphoreType.DMA((32,)),
            pltpu.SemaphoreType.DMA((32,)),
            pltpu.SemaphoreType.DMA((2, STEPS, CHUNKS)),
            pltpu.SemaphoreType.DMA((2, STEPS, CHUNKS)),
            pltpu.SemaphoreType.DMA((3,)),
            pltpu.SemaphoreType.DMA((3,)),
            pltpu.SemaphoreType.DMA((stages,)),
            pltpu.SemaphoreType.DMA((stages,)),
        ],
        compiler_params=pltpu.CompilerParams(
            collective_id=0, has_side_effects=True, vmem_limit_bytes=48 * 1024 * 1024
        ),
    )(
        *(
            pltpu.with_memory_space_constraint(x, pltpu.HBM)
            for x in (
                adjoint_now,
                adjoint_later,
                courant,
                checkpoint_codes,
                scale_index,
                receiver_cell,
                observed,
                scale_table,
                source_cell,
            )
        )
    )
    gradient, first, second, misfit = pl.pallas_call(
        finish,
        out_shape=tuple(
            jax.ShapeDtypeStruct(x.shape if i < 3 else (1, 1), f32) for i, x in enumerate(results)
        ),
        in_specs=[whole] * 4,
        out_specs=[outside] * 4,
        scratch_shapes=[
            pltpu.VMEM((8, LANES), f32),
            pltpu.VMEM((1, 1), f32),
            pltpu.SemaphoreType.DMA((5,)),
        ],
        compiler_params=pltpu.CompilerParams(vmem_limit_bytes=1024 * 1024),
    )(*results)
    return gradient, first, second, misfit.reshape(())


def solution(mesh):
    sizes = dict(mesh.shape)
    return jax.shard_map(
        functools.partial(body, sizes["space"], sizes["shot"]),
        mesh=mesh,
        in_specs=(
            P("shot", "space", None, None),
            P("shot", "space", None, None),
            P("space", None, None),
            P("shot", None, "space", None, None),
            P("shot", None, "space", None),
            P(),
            P("shot", "space"),
            P("shot", None, "space"),
            P("shot", None),
        ),
        out_specs=(
            P("space", "shot", None),
            P("shot", "space", None, None),
            P("shot", "space", None, None),
            P(),
        ),
        check_vma=False,
    )
```

```python
import functools

import jax
import jax.numpy as jnp
from jax import lax
from jax.experimental import pallas as pl
from jax.experimental.pallas import tpu as pltpu
from jax.sharding import PartitionSpec as P

STEPS = 4
MUTE = 8
RADIUS = 4
LANES = 128
PAD = 8
CHUNKS = 4
COEFFS = (-205.0 / 72.0, 8.0 / 5.0, -1.0 / 5.0, 8.0 / 315.0, -1.0 / 560.0)
MESH = pl.DeviceIdType.MESH


def kernel(
    space_size,
    shot_size,
    now_hbm,
    later_hbm,
    courant_hbm,
    codes_hbm,
    index_hbm,
    cells_hbm,
    observed_hbm,
    table_hbm,
    source_hbm,
    grad_hbm,
    first_hbm,
    second_hbm,
    misfit_hbm,
    table,
    source_ref,
    field,
    courant,
    words,
    index,
    cells,
    observed,
    scales,
    flipped,
    spread,
    rows_hot,
    cols_hot,
    values,
    injected,
    scale_at,
    image,
    from_sibling,
    combined,
    from_partner,
    grad_out,
    sums,
    sums_in,
    gathered,
    ordered,
    load_sem,
    out_sem,
    halo_send,
    halo_recv,
    image_send,
    image_recv,
    sum_send,
    sum_recv,
    met,
):
    scale = 0.5 / (shot_size * STEPS * cells.shape[1] * space_size)
    depth = courant.shape[1]
    height = courant.shape[2]
    tall = height // CHUNKS
    receivers = cells.shape[1]
    me = lax.axis_index("space")
    shot = lax.axis_index("shot")
    side, core = shot // 2, shot % 2
    up, down = (me + 1) % space_size, (me + space_size - 1) % space_size
    sibling = shot + 1 - 2 * core
    partner = (shot + 2) % 4

    peers = [{"space": up}, {"space": down}, {"shot": sibling}, {"shot": partner}]
    barrier = pltpu.get_barrier_semaphore()
    for peer in peers:
        pl.semaphore_signal(barrier, inc=1, device_id=peer, device_id_type=MESH)

    stages = [{"shot": sibling}, {"shot": partner}]
    hello = [None, None]
    windows = [None, None]
    bit = 1
    while bit < space_size:
        stages.append({"space": (me + bit) % space_size})
        hello.append({"space": (me + space_size - bit) % space_size})
        windows.append(bit)
        bit *= 2

    loads = []

    def load(src, dst):
        copy = pltpu.make_async_copy(src, dst, load_sem.at[len(loads)])
        copy.start()
        loads.append(copy)
        return copy

    def lanes(xc):
        return pl.ds(xc * LANES, LANES)

    edges = []
    for xc in range(4):
        for z in (0, depth - RADIUS):
            edges.append(
                load(
                    now_hbm.at[0, pl.ds(z, RADIUS), :, lanes(xc)],
                    field.at[1, xc, pl.ds(RADIUS + z, RADIUS), pl.ds(PAD, height), :],
                )
            )
    small = [
        load(index_hbm.at[0], index),
        load(cells_hbm, cells),
        load(observed_hbm.at[0], observed),
        load(table_hbm, table),
        load(source_hbm, source_ref),
    ]
    small_words = load(codes_hbm.at[0], words)
    rest = []
    for xc in range(4):
        rest.append(
            load(
                now_hbm.at[0, pl.ds(RADIUS, depth - 2 * RADIUS), :, lanes(xc)],
                field.at[1, xc, pl.ds(2 * RADIUS, depth - 2 * RADIUS), pl.ds(PAD, height), :],
            )
        )
        rest.append(
            load(
                later_hbm.at[0, :, :, lanes(xc)],
                field.at[0, xc, pl.ds(RADIUS, depth), pl.ds(PAD, height), :],
            )
        )
        rest.append(load(courant_hbm.at[:, :, lanes(xc)], courant.at[xc]))

    pl.semaphore_wait(barrier, len(peers))

    def rows_of(n):
        c = (n + 2 * (1 - side)) % CHUNKS
        return c, pl.multiple_of(PAD + c * tall, 8)

    def halo_copy(t, n, way):
        _, row = rows_of(n)
        src_z, dst_z, target = ((depth, 0, up), (RADIUS, RADIUS + depth, down))[way]
        return pltpu.make_async_remote_copy(
            src_ref=field.at[1 + t, :, pl.ds(src_z, RADIUS), pl.ds(row, tall), :],
            dst_ref=field.at[1 + t, :, pl.ds(dst_z, RADIUS), pl.ds(row, tall), :],
            send_sem=halo_send.at[way, t, n],
            recv_sem=halo_recv.at[way, t, n],
            device_id={"space": target},
            device_id_type=MESH,
        )

    has_up = me < space_size - 1
    has_down = me > 0

    def send_halo(t, n):
        @pl.when(has_up)
        def _():
            halo_copy(t, n, 0).start()

        @pl.when(has_down)
        def _():
            halo_copy(t, n, 1).start()

    for copy in edges:
        copy.wait()

    def first_sends(n, carry):
        send_halo(0, n)
        return carry

    lax.fori_loop(0, CHUNKS, first_sends, 0)

    zero_rows = jnp.zeros((4, 1, PAD, LANES), jnp.float32)

    def clear_rows(i, carry):
        level = 1 + i // depth
        z = RADIUS + i % depth
        field[pl.ds(level, 1), :, pl.ds(z, 1), pl.ds(0, PAD), :] = zero_rows[None]
        field[pl.ds(level, 1), :, pl.ds(z, 1), pl.ds(PAD + height, PAD), :] = zero_rows[None]
        return carry

    lax.fori_loop(0, STEPS * depth, clear_rows, 0)
    zero_plane = jnp.zeros((1, 4, 1, height, LANES), jnp.float32)

    @pl.when(me == 0)
    def _():
        def clear(i, carry):
            field[pl.ds(1 + i // RADIUS, 1), :, pl.ds(i % RADIUS, 1), pl.ds(PAD, height), :] = (
                zero_plane
            )
            return carry

        lax.fori_loop(0, STEPS * RADIUS, clear, 0)

    @pl.when(me == space_size - 1)
    def _():
        def clear(i, carry):
            field[
                pl.ds(1 + i // RADIUS, 1),
                :,
                pl.ds(RADIUS + depth + i % RADIUS, 1),
                pl.ds(PAD, height),
                :,
            ] = zero_plane
            return carry

        lax.fori_loop(0, STEPS * RADIUS, clear, 0)

    for copy in small:
        copy.wait()
    source = [source_ref[0, i] for i in range(3)]
    levels = index.shape[0]
    flat_index = index[...].reshape(levels * depth, index.shape[2])

    def look_up(k, acc):
        return jnp.where(flat_index == k, table[k], acc)

    looked = lax.fori_loop(0, table.shape[0], look_up, jnp.zeros(flat_index.shape, jnp.float32))
    scales[pl.ds(0, levels * depth), :] = looked
    scales[pl.ds(levels * depth, LANES - levels * depth), :] = jnp.zeros(
        (LANES - levels * depth, index.shape[2]), jnp.float32
    )
    flipped[...] = scales[...].T
    width = 4 * LANES
    cell = cells[...] - me * (depth * height * width)
    row_of = cell // width
    col_of = cell % width
    block_of = (cell // LANES) % (4 * height)
    slab_of = row_of // height
    for z in range(depth):
        ids = z * height + lax.broadcasted_iota(jnp.int32, (height, receivers), 0)
        rows_hot[z] = jnp.where(ids == row_of, 1.0, 0.0).astype(jnp.bfloat16)
    col_ids = lax.broadcasted_iota(jnp.int32, (width, receivers), 0)
    cols_hot[...] = jnp.where(col_ids == col_of, 1.0, 0.0).astype(jnp.bfloat16)
    block_ids = lax.broadcasted_iota(jnp.int32, (4 * height, receivers), 0)
    blocks_hot = jnp.where(block_ids == block_of, 1.0, 0.0)
    scale_at[...] = jnp.dot(
        scales[...], blocks_hot, precision=lax.Precision.HIGHEST, preferred_element_type=jnp.float32
    )
    depth_ids = lax.broadcasted_iota(jnp.int32, (depth, receivers), 0)
    small_words.wait()
    planes = 4

    def residuals(t):
        level = STEPS - t

        def gather(i, acc):
            w = words[level, pl.ds(i * planes, planes), :, :].reshape(planes * height, LANES)
            parts = [
                (((w >> (8 * m)) & 255) - 128).astype(jnp.float32).astype(jnp.bfloat16)
                for m in range(4)
            ]
            found = jnp.dot(
                jnp.concatenate(parts, axis=1), cols_hot[...], preferred_element_type=jnp.float32
            )
            hot = rows_hot[pl.ds(i * planes, planes), :, :].reshape(planes * height, receivers)
            return acc + jnp.sum(found * hot.astype(jnp.float32), axis=0, keepdims=True)

        code = lax.fori_loop(0, depth // planes, gather, jnp.zeros((1, receivers), jnp.float32))
        part = scale_at[pl.ds(level * depth, depth), :]
        factor = jnp.sum(jnp.where(depth_ids == slab_of, part, 0.0), axis=0, keepdims=True)
        residual = code * factor - observed[level - 1 : level, :]
        squares = jnp.broadcast_to(
            jnp.sum(residual * residual, axis=1, keepdims=True), sums.shape[1:]
        )
        sums[0] = squares if t == 0 else sums[0] + squares
        left = residual
        for piece in range(3):
            short = left.astype(jnp.bfloat16).astype(jnp.float32)
            left = left - short
            values[t, piece] = jnp.where(col_ids == col_of, short, 0.0).astype(jnp.bfloat16)

    residuals(0)

    def end_stage(b):
        sum_copy(b).wait_recv()
        if hello[b] is not None:
            pl.semaphore_wait(met.at[b], 1)
        else:
            both = sums[b] + sums_in[b]
            sums[b + 1] = both
            if windows[b + 1] is not None:
                gathered[0] = both[0:1]

    def sum_copy(b):
        bit = windows[b]
        return pltpu.make_async_remote_copy(
            src_ref=sums.at[b] if bit is None else gathered.at[pl.ds(0, bit)],
            dst_ref=sums_in.at[b] if bit is None else gathered.at[pl.ds(bit, bit)],
            send_sem=sum_send.at[b],
            recv_sem=sum_recv.at[b],
            device_id=stages[b],
            device_id_type=MESH,
        )

    for copy in rest:
        copy.wait()

    lane = lax.broadcasted_iota(jnp.int32, (tall, LANES), 1)

    def update(t, c, row, z):
        def at(xc, dz, dy):
            return field[1 + t, xc, RADIUS + z + dz, pl.ds(row + dy, tall), :]

        centre = [at(xc, 0, 0) for xc in range(4)]
        after = [[pltpu.roll(v, LANES - i, 1) for v in centre] for i in range(1, 5)]
        before = [[pltpu.roll(v, i, 1) for v in centre] for i in range(1, 5)]
        for xc in range(4):
            acc = (3.0 * COEFFS[0]) * centre[xc]
            for i in range(1, 5):
                nxt = after[i - 1][xc + 1] if xc < 3 else 0.0
                prv = before[i - 1][xc - 1] if xc > 0 else 0.0
                pair = jnp.where(lane < LANES - i, after[i - 1][xc], nxt) + jnp.where(
                    lane >= i, before[i - 1][xc], prv
                )
                pair = pair + (at(xc, i, 0) + at(xc, -i, 0)) + (at(xc, 0, i) + at(xc, 0, -i))
                acc = acc + COEFFS[i] * pair
            y0 = pl.multiple_of(row - PAD, 8)
            old = field[t, xc, RADIUS + z, pl.ds(row, tall), :]
            new = 2.0 * centre[xc] - old + courant[xc, z, pl.ds(y0, tall), :] * acc
            field[(2 + t) % (STEPS + 1), xc, RADIUS + z, pl.ds(row, tall), :] = (
                new + injected[xc, z, :, :]
            )

    def inject(t, c):
        hot = rows_hot[:, pl.ds(pl.multiple_of(c * tall, 16), tall), :].reshape(
            depth * tall, receivers
        )
        acc = None
        for piece in range(3):
            term = lax.dot_general(
                hot,
                values[t, piece],
                (((1,), (1,)), ((), ())),
                preferred_element_type=jnp.float32,
            )
            acc = term if acc is None else acc + term
        for xc in range(4):
            injected[xc] = acc[:, xc * LANES : (xc + 1) * LANES].reshape(depth, tall, LANES)

    def spread_rows(c):
        row = pl.multiple_of(c * tall, 8)
        columns = [
            flipped[pl.ds(pl.multiple_of(4 * c * tall, 8) + m, tall, stride=4), :]
            for m in range(4)
        ]
        for i in range(levels * depth):
            for m in range(4):
                spread[i // depth, i % depth, m, pl.ds(row, tall), :] = jnp.broadcast_to(
                    columns[m][:, i : i + 1], (tall, LANES)
                )

    def add_image(t, c, row, first):
        level = STEPS - t
        y0 = pl.multiple_of(row - PAD, 8)

        def plane(z, carry):
            ws = [words[level + d, z, pl.ds(y0, tall), :] for d in (-1, 0, 1)]
            for m in range(4):
                f = [
                    (((w >> (8 * m)) & 255) - 128).astype(jnp.float32)
                    * spread[level + d, z, m, pl.ds(y0, tall), :]
                    for w, d in zip(ws, (-1, 0, 1))
                ]
                term = field[1 + t, m, RADIUS + z, pl.ds(row, tall), :] * (
                    f[2] - 2.0 * f[1] + f[0]
                )
                if first:
                    image[c, m, z] = term
                else:
                    image[c, m, z] = image[c, m, z] + term
            return carry

        lax.fori_loop(0, depth, plane, 0)

    def mute(c):
        y = c * tall + lax.broadcasted_iota(jnp.int32, (tall, LANES), 0)
        across = [(y - source[1]) ** 2 + (m * LANES + lane - source[2]) ** 2 for m in range(4)]

        def plane(z, carry):
            dz = me * depth + z - source[0]
            for m in range(4):
                dist = (across[m] + dz * dz).astype(jnp.float32)
                image[c, m, z] = image[c, m, z] * (1.0 - jnp.exp(-dist / (2.0 * MUTE * MUTE)))
            return carry

        lax.fori_loop(0, depth, plane, 0)

    far = 2 * (1 - side) + core
    near = shot

    def pair_copy(c, slot):
        return pltpu.make_async_remote_copy(
            src_ref=image.at[c],
            dst_ref=from_sibling.at[slot],
            send_sem=image_send.at[slot],
            recv_sem=image_recv.at[slot],
            device_id={"shot": sibling},
            device_id_type=MESH,
        )

    sibling_far = 2 * (1 - side) + 1 - core
    far_copy = pair_copy(sibling_far, 0)
    near_copy = pair_copy(sibling, 1)
    partner_copy = pltpu.make_async_remote_copy(
        src_ref=combined,
        dst_ref=from_partner,
        send_sem=image_send.at[2],
        recv_sem=image_recv.at[2],
        device_id={"shot": partner},
        device_id_type=MESH,
    )

    outs = []

    def store(src, dst):
        copy = pltpu.make_async_copy(src, dst, out_sem.at[len(outs)])
        copy.start()
        outs.append(copy)

    def first_copy(n, xc):
        c, row = rows_of(n)
        return pltpu.make_async_copy(
            field.at[0, xc, pl.ds(RADIUS, depth), pl.ds(row, tall), :],
            first_hbm.at[0, :, pl.ds(pl.multiple_of(row - PAD, 8), tall), lanes(xc)],
            out_sem.at[16 + n * 4 + xc],
        )

    for t in range(STEPS):

        def task(n, carry, t=t):
            c, row = rows_of(n)
            if t in (1, 2):
                for j in range(4):
                    b = 4 * (t - 1) + j

                    @pl.when(n == j)
                    def _():
                        if b > 0:
                            end_stage(b - 1)
                        sum_copy(b).start()
                        if hello[b] is not None:
                            pl.semaphore_signal(
                                met.at[b], inc=1, device_id=hello[b], device_id_type=MESH
                            )

            inject(t, c)

            def inner(z, carry):
                update(t, c, row, z)
                return carry

            lax.fori_loop(RADIUS, depth - RADIUS, inner, 0)
            if t == 3:

                @pl.when(n == 0)
                def _():
                    far_copy.wait_recv()

                    def plane(z, carry):
                        for m in range(4):
                            combined[m, z] = image[far, m, z] + from_sibling[0, m, z]
                        return carry

                    lax.fori_loop(0, depth, plane, 0)
                    partner_copy.start()

            @pl.when(has_down)
            def _():
                halo_copy(t, n, 0).wait_recv()

            lax.fori_loop(0, RADIUS, inner, 0)
            if t < STEPS - 1:

                @pl.when(has_down)
                def _():
                    halo_copy(t + 1, n, 1).start()

            @pl.when(has_up)
            def _():
                halo_copy(t, n, 1).wait_recv()

            lax.fori_loop(depth - RADIUS, depth, inner, 0)
            if t < STEPS - 1:

                @pl.when(has_up)
                def _():
                    halo_copy(t + 1, n, 0).start()

            if t == 0:
                for j in range(1, STEPS):

                    @pl.when(n == j - 1)
                    def _():
                        residuals(j)

            if t == 1:
                spread_rows(c)
                add_image(0, c, row, True)
                add_image(1, c, row, False)
            if t == 2:
                add_image(2, c, row, False)
                add_image(3, c, row, False)
            if t == STEPS - 1:
                for xc in range(4):
                    first_copy(n, xc).start()
            if t == 2:
                mute(c)

                @pl.when(c == sibling_far)
                def _():
                    far_copy.start()

                @pl.when(c == sibling)
                def _():
                    near_copy.start()

            return carry

        lax.fori_loop(0, CHUNKS, task, 0)
        if t == 2:
            last = len(stages) - 1
            end_stage(last)

            def place(k, carry):
                ordered[pl.ds((me + space_size - k) % space_size, 1)] = gathered[pl.ds(k, 1)]
                return carry

            lax.fori_loop(0, space_size, place, 0)
            everyone = jnp.sum(ordered[...], axis=0) * scale
            sums[3] = jnp.broadcast_to(everyone, sums.shape[1:])
        if t == 2:
            for xc in range(4):
                store(
                    field.at[STEPS, xc, pl.ds(RADIUS, depth), pl.ds(PAD, height), :],
                    second_hbm.at[0, :, :, lanes(xc)],
                )
            store(sums.at[3], misfit_hbm)
    near_copy.wait_recv()
    partner_copy.wait_recv()

    def plane(z, carry):
        for m in range(4):
            grad_out[m, z] = (
                image[near, m, z] + from_sibling[1, m, z] + from_partner[m, z]
            )
        return carry

    lax.fori_loop(0, depth, plane, 0)
    for xc in range(4):
        store(grad_out.at[xc], grad_hbm.at[:, :, lanes(xc)])

    def drain(n, carry):
        for t in range(STEPS):

            @pl.when(has_up)
            def _():
                halo_copy(t, n, 0).wait_send()

            @pl.when(has_down)
            def _():
                halo_copy(t, n, 1).wait_send()

        for xc in range(4):
            first_copy(n, xc).wait()
        return carry

    far_copy.wait_send()
    near_copy.wait_send()
    partner_copy.wait_send()
    for b in range(len(stages)):
        sum_copy(b).wait_send()
    lax.fori_loop(0, CHUNKS, drain, 0)
    for copy in outs:
        copy.wait()


def finish(g_in, f_in, s_in, m_in, g_out, f_out, s_out, m_out, tile, one, sem):
    pairs = [(m_in, tile), (f_in, f_out), (s_in, s_out), (g_in, g_out)]
    copies = [pltpu.make_async_copy(a, b, sem.at[i]) for i, (a, b) in enumerate(pairs)]
    for copy in copies:
        copy.start()
    copies[0].wait()
    one[...] = tile[0:1, 0:1]
    last = pltpu.make_async_copy(one, m_out, sem.at[len(pairs)])
    last.start()
    for copy in copies[1:]:
        copy.wait()
    last.wait()


def body(
    space_size,
    shot_size,
    adjoint_now,
    adjoint_later,
    courant,
    checkpoint_codes,
    scale_index,
    scale_table,
    receiver_cell,
    observed,
    source_cell,
):
    _, depth, height, width = adjoint_now.shape
    levels = checkpoint_codes.shape[1]
    receivers = receiver_cell.shape[1]
    tall = height // CHUNKS
    quarter = (4, depth, tall, LANES)
    stages = (space_size * shot_size).bit_length() - 1
    whole = pl.BlockSpec(memory_space=pl.ANY)
    outside = pl.BlockSpec(memory_space=pltpu.HBM)
    f32 = jnp.float32
    results = pl.pallas_call(
        functools.partial(kernel, space_size, shot_size),
        out_shape=(
            jax.ShapeDtypeStruct((depth, tall, width), f32),
            jax.ShapeDtypeStruct(adjoint_now.shape, f32),
            jax.ShapeDtypeStruct(adjoint_now.shape, f32),
            jax.ShapeDtypeStruct((8, LANES), f32),
        ),
        in_specs=[outside] * 9,
        out_specs=[whole] * 4,
        scratch_shapes=[
            pltpu.SMEM(scale_table.shape, f32),
            pltpu.SMEM(source_cell.shape, jnp.int32),
            pltpu.VMEM((STEPS + 1, 4, depth + 2 * RADIUS, height + 2 * PAD, LANES), f32),
            pltpu.VMEM((4, depth, height, LANES), f32),
            pltpu.VMEM((levels, depth, height, LANES), jnp.int32),
            pltpu.VMEM((levels, depth, 4 * height), jnp.int32),
            pltpu.VMEM((1, receivers), jnp.int32),
            pltpu.VMEM((STEPS, receivers), f32),
            pltpu.VMEM((LANES, 4 * height), f32),
            pltpu.VMEM((4 * height, LANES), f32),
            pltpu.VMEM((levels, depth, 4, height, LANES), f32),
            pltpu.VMEM((depth, height, receivers), jnp.bfloat16),
            pltpu.VMEM((width, receivers), jnp.bfloat16),
            pltpu.VMEM((STEPS, 3, width, receivers), jnp.bfloat16),
            pltpu.VMEM(quarter, f32),
            pltpu.VMEM((LANES, receivers), f32),
            pltpu.VMEM((CHUNKS, *quarter), f32),
            pltpu.VMEM((2, *quarter), f32),
            pltpu.VMEM(quarter, f32),
            pltpu.VMEM(quarter, f32),
            pltpu.VMEM(quarter, f32),
            pltpu.VMEM((4, 8, LANES), f32),
            pltpu.VMEM((2, 8, LANES), f32),
            pltpu.VMEM((space_size, 1, LANES), f32),
            pltpu.VMEM((space_size, 1, LANES), f32),
            pltpu.SemaphoreType.DMA((32,)),
            pltpu.SemaphoreType.DMA((32,)),
            pltpu.SemaphoreType.DMA((2, STEPS, CHUNKS)),
            pltpu.SemaphoreType.DMA((2, STEPS, CHUNKS)),
            pltpu.SemaphoreType.DMA((3,)),
            pltpu.SemaphoreType.DMA((3,)),
            pltpu.SemaphoreType.DMA((stages,)),
            pltpu.SemaphoreType.DMA((stages,)),
            pltpu.SemaphoreType.REGULAR((stages,)),
        ],
        compiler_params=pltpu.CompilerParams(
            collective_id=0, has_side_effects=True, vmem_limit_bytes=48 * 1024 * 1024
        ),
    )(
        *(
            pltpu.with_memory_space_constraint(x, pltpu.HBM)
            for x in (
                adjoint_now,
                adjoint_later,
                courant,
                checkpoint_codes,
                scale_index,
                receiver_cell,
                observed,
                scale_table,
                source_cell,
            )
        )
    )
    gradient, first, second, misfit = pl.pallas_call(
        finish,
        out_shape=tuple(
            jax.ShapeDtypeStruct(x.shape if i < 3 else (1, 1), f32) for i, x in enumerate(results)
        ),
        in_specs=[whole] * 4,
        out_specs=[outside] * 4,
        scratch_shapes=[
            pltpu.VMEM((8, LANES), f32),
            pltpu.VMEM((1, 1), f32),
            pltpu.SemaphoreType.DMA((5,)),
        ],
        compiler_params=pltpu.CompilerParams(vmem_limit_bytes=1024 * 1024),
    )(*results)
    return gradient, first, second, misfit.reshape(())


def solution(mesh):
    sizes = dict(mesh.shape)
    return jax.shard_map(
        functools.partial(body, sizes["space"], sizes["shot"]),
        mesh=mesh,
        in_specs=(
            P("shot", "space", None, None),
            P("shot", "space", None, None),
            P("space", None, None),
            P("shot", None, "space", None, None),
            P("shot", None, "space", None),
            P(),
            P("shot", "space"),
            P("shot", None, "space"),
            P("shot", None),
        ),
        out_specs=(
            P("space", "shot", None),
            P("shot", "space", None, None),
            P("shot", "space", None, None),
            P(),
        ),
        check_vma=False,
    )
```

```python
import functools

import jax
import jax.numpy as jnp
from jax import lax
from jax.experimental import pallas as pl
from jax.experimental.pallas import tpu as pltpu
from jax.sharding import PartitionSpec as P

STEPS = 4
MUTE = 8
RADIUS = 4
LANES = 128
PAD = 8
CHUNKS = 4
COEFFS = (-205.0 / 72.0, 8.0 / 5.0, -1.0 / 5.0, 8.0 / 315.0, -1.0 / 560.0)
MESH = pl.DeviceIdType.MESH


def kernel(
    space_size,
    shot_size,
    now_hbm,
    later_hbm,
    courant_hbm,
    codes_hbm,
    index_hbm,
    cells_hbm,
    observed_hbm,
    table_hbm,
    source_hbm,
    grad_hbm,
    first_hbm,
    second_hbm,
    misfit_hbm,
    table,
    source_ref,
    field,
    courant,
    words,
    index,
    cells,
    observed,
    scales,
    flipped,
    spread,
    rows_hot,
    cols_hot,
    values,
    injected,
    scale_at,
    image,
    from_sibling,
    combined,
    from_partner,
    grad_out,
    sums,
    sums_in,
    gathered,
    ordered,
    load_sem,
    out_sem,
    halo_send,
    halo_recv,
    image_send,
    image_recv,
    sum_send,
    sum_recv,
    met,
):
    scale = 0.5 / (shot_size * STEPS * cells.shape[1] * space_size)
    depth = courant.shape[1]
    height = courant.shape[2]
    tall = height // CHUNKS
    receivers = cells.shape[1]
    me = lax.axis_index("space")
    shot = lax.axis_index("shot")
    side, core = shot // 2, shot % 2
    up, down = (me + 1) % space_size, (me + space_size - 1) % space_size
    sibling = shot + 1 - 2 * core
    partner = (shot + 2) % 4

    peers = [{"space": up}, {"space": down}, {"shot": sibling}, {"shot": partner}]
    barrier = pltpu.get_barrier_semaphore()
    for peer in peers:
        pl.semaphore_signal(barrier, inc=1, device_id=peer, device_id_type=MESH)

    stages = [{"shot": sibling}, {"shot": partner}]
    hello = [None, None]
    windows = [None, None]
    bit = 1
    while bit < space_size:
        stages.append({"space": (me + bit) % space_size})
        hello.append({"space": (me + space_size - bit) % space_size})
        windows.append(bit)
        bit *= 2

    loads = []

    def load(src, dst):
        copy = pltpu.make_async_copy(src, dst, load_sem.at[len(loads)])
        copy.start()
        loads.append(copy)
        return copy

    def lanes(xc):
        return pl.ds(xc * LANES, LANES)

    edges = []
    for xc in range(4):
        for z in (0, depth - RADIUS):
            edges.append(
                load(
                    now_hbm.at[0, pl.ds(z, RADIUS), :, lanes(xc)],
                    field.at[1, xc, pl.ds(RADIUS + z, RADIUS), pl.ds(PAD, height), :],
                )
            )
    small = [
        load(index_hbm.at[0], index),
        load(cells_hbm, cells),
        load(observed_hbm.at[0], observed),
        load(table_hbm, table),
        load(source_hbm, source_ref),
    ]
    small_words = load(codes_hbm.at[0], words)
    rest = []
    for xc in range(4):
        rest.append(
            load(
                now_hbm.at[0, pl.ds(RADIUS, depth - 2 * RADIUS), :, lanes(xc)],
                field.at[1, xc, pl.ds(2 * RADIUS, depth - 2 * RADIUS), pl.ds(PAD, height), :],
            )
        )
        rest.append(
            load(
                later_hbm.at[0, :, :, lanes(xc)],
                field.at[0, xc, pl.ds(RADIUS, depth), pl.ds(PAD, height), :],
            )
        )
        rest.append(load(courant_hbm.at[:, :, lanes(xc)], courant.at[xc]))

    pl.semaphore_wait(barrier, len(peers))

    def rows_of(n):
        c = (n + 2 * (1 - side)) % CHUNKS
        return c, pl.multiple_of(PAD + c * tall, 8)

    def halo_copy(t, n, way):
        _, row = rows_of(n)
        src_z, dst_z, target = ((depth, 0, up), (RADIUS, RADIUS + depth, down))[way]
        return pltpu.make_async_remote_copy(
            src_ref=field.at[1 + t, :, pl.ds(src_z, RADIUS), pl.ds(row, tall), :],
            dst_ref=field.at[1 + t, :, pl.ds(dst_z, RADIUS), pl.ds(row, tall), :],
            send_sem=halo_send.at[way, t, n],
            recv_sem=halo_recv.at[way, t, n],
            device_id={"space": target},
            device_id_type=MESH,
        )

    has_up = me < space_size - 1
    has_down = me > 0

    def send_halo(t, n):
        @pl.when(has_up)
        def _():
            halo_copy(t, n, 0).start()

        @pl.when(has_down)
        def _():
            halo_copy(t, n, 1).start()

    for copy in edges:
        copy.wait()

    def first_sends(n, carry):
        send_halo(0, n)
        return carry

    lax.fori_loop(0, CHUNKS, first_sends, 0)

    zero_rows = jnp.zeros((4, 1, PAD, LANES), jnp.float32)

    def clear_rows(i, carry):
        level = 1 + i // depth
        z = RADIUS + i % depth
        field[pl.ds(level, 1), :, pl.ds(z, 1), pl.ds(0, PAD), :] = zero_rows[None]
        field[pl.ds(level, 1), :, pl.ds(z, 1), pl.ds(PAD + height, PAD), :] = zero_rows[None]
        return carry

    lax.fori_loop(0, STEPS * depth, clear_rows, 0)
    zero_plane = jnp.zeros((1, 4, 1, height, LANES), jnp.float32)

    @pl.when(me == 0)
    def _():
        def clear(i, carry):
            field[pl.ds(1 + i // RADIUS, 1), :, pl.ds(i % RADIUS, 1), pl.ds(PAD, height), :] = (
                zero_plane
            )
            return carry

        lax.fori_loop(0, STEPS * RADIUS, clear, 0)

    @pl.when(me == space_size - 1)
    def _():
        def clear(i, carry):
            field[
                pl.ds(1 + i // RADIUS, 1),
                :,
                pl.ds(RADIUS + depth + i % RADIUS, 1),
                pl.ds(PAD, height),
                :,
            ] = zero_plane
            return carry

        lax.fori_loop(0, STEPS * RADIUS, clear, 0)

    for copy in small:
        copy.wait()
    source = [source_ref[0, i] for i in range(3)]
    levels = index.shape[0]
    flat_index = index[...].reshape(levels * depth, index.shape[2])

    def look_up(k, acc):
        return jnp.where(flat_index == k, table[k], acc)

    looked = lax.fori_loop(0, table.shape[0], look_up, jnp.zeros(flat_index.shape, jnp.float32))
    scales[pl.ds(0, levels * depth), :] = looked
    scales[pl.ds(levels * depth, LANES - levels * depth), :] = jnp.zeros(
        (LANES - levels * depth, index.shape[2]), jnp.float32
    )
    flipped[...] = scales[...].T
    width = 4 * LANES
    cell = cells[...] - me * (depth * height * width)
    row_of = cell // width
    col_of = cell % width
    block_of = (cell // LANES) % (4 * height)
    slab_of = row_of // height
    for z in range(depth):
        ids = z * height + lax.broadcasted_iota(jnp.int32, (height, receivers), 0)
        rows_hot[z] = jnp.where(ids == row_of, 1.0, 0.0).astype(jnp.bfloat16)
    col_ids = lax.broadcasted_iota(jnp.int32, (width, receivers), 0)
    cols_hot[...] = jnp.where(col_ids == col_of, 1.0, 0.0).astype(jnp.bfloat16)
    block_ids = lax.broadcasted_iota(jnp.int32, (4 * height, receivers), 0)
    blocks_hot = jnp.where(block_ids == block_of, 1.0, 0.0)
    scale_at[...] = jnp.dot(
        scales[...], blocks_hot, precision=lax.Precision.HIGHEST, preferred_element_type=jnp.float32
    )
    depth_ids = lax.broadcasted_iota(jnp.int32, (depth, receivers), 0)
    small_words.wait()
    planes = 4

    def residuals(t):
        level = STEPS - t

        def gather(i, acc):
            w = words[level, pl.ds(i * planes, planes), :, :].reshape(planes * height, LANES)
            parts = [
                (((w >> (8 * m)) & 255) - 128).astype(jnp.float32).astype(jnp.bfloat16)
                for m in range(4)
            ]
            found = jnp.dot(
                jnp.concatenate(parts, axis=1), cols_hot[...], preferred_element_type=jnp.float32
            )
            hot = rows_hot[pl.ds(i * planes, planes), :, :].reshape(planes * height, receivers)
            return acc + jnp.sum(found * hot.astype(jnp.float32), axis=0, keepdims=True)

        code = lax.fori_loop(0, depth // planes, gather, jnp.zeros((1, receivers), jnp.float32))
        part = scale_at[pl.ds(level * depth, depth), :]
        factor = jnp.sum(jnp.where(depth_ids == slab_of, part, 0.0), axis=0, keepdims=True)
        residual = code * factor - observed[level - 1 : level, :]
        squares = jnp.broadcast_to(
            jnp.sum(residual * residual, axis=1, keepdims=True), sums.shape[1:]
        )
        sums[0] = squares if t == 0 else sums[0] + squares
        left = residual
        for piece in range(3):
            short = left.astype(jnp.bfloat16).astype(jnp.float32)
            left = left - short
            values[t, piece] = jnp.where(col_ids == col_of, short, 0.0).astype(jnp.bfloat16)

    residuals(0)

    def end_stage(b):
        sum_copy(b).wait_recv()
        if hello[b] is not None:
            pl.semaphore_wait(met.at[b], 1)
        else:
            both = sums[b] + sums_in[b]
            sums[b + 1] = both
            if windows[b + 1] is not None:
                gathered[0] = both[0:1]

    def sum_copy(b):
        bit = windows[b]
        return pltpu.make_async_remote_copy(
            src_ref=sums.at[b] if bit is None else gathered.at[pl.ds(0, bit)],
            dst_ref=sums_in.at[b] if bit is None else gathered.at[pl.ds(bit, bit)],
            send_sem=sum_send.at[b],
            recv_sem=sum_recv.at[b],
            device_id=stages[b],
            device_id_type=MESH,
        )

    for copy in rest:
        copy.wait()

    lane = lax.broadcasted_iota(jnp.int32, (tall, LANES), 1)

    def update(t, c, row, z):
        def at(xc, dz, dy):
            return field[1 + t, xc, RADIUS + z + dz, pl.ds(row + dy, tall), :]

        centre = [at(xc, 0, 0) for xc in range(4)]
        after = [[pltpu.roll(v, LANES - i, 1) for v in centre] for i in range(1, 5)]
        before = [[pltpu.roll(v, i, 1) for v in centre] for i in range(1, 5)]
        for xc in range(4):
            acc = (3.0 * COEFFS[0]) * centre[xc]
            for i in range(1, 5):
                nxt = after[i - 1][xc + 1] if xc < 3 else 0.0
                prv = before[i - 1][xc - 1] if xc > 0 else 0.0
                pair = jnp.where(lane < LANES - i, after[i - 1][xc], nxt) + jnp.where(
                    lane >= i, before[i - 1][xc], prv
                )
                pair = pair + (at(xc, i, 0) + at(xc, -i, 0)) + (at(xc, 0, i) + at(xc, 0, -i))
                acc = acc + COEFFS[i] * pair
            y0 = pl.multiple_of(row - PAD, 8)
            old = field[t, xc, RADIUS + z, pl.ds(row, tall), :]
            new = 2.0 * centre[xc] - old + courant[xc, z, pl.ds(y0, tall), :] * acc
            field[(2 + t) % (STEPS + 1), xc, RADIUS + z, pl.ds(row, tall), :] = (
                new + injected[xc, z, :, :]
            )

    def inject(t, c):
        hot = rows_hot[:, pl.ds(pl.multiple_of(c * tall, 16), tall), :].reshape(
            depth * tall, receivers
        )
        acc = None
        for piece in range(3):
            term = lax.dot_general(
                hot,
                values[t, piece],
                (((1,), (1,)), ((), ())),
                preferred_element_type=jnp.float32,
            )
            acc = term if acc is None else acc + term
        for xc in range(4):
            injected[xc] = acc[:, xc * LANES : (xc + 1) * LANES].reshape(depth, tall, LANES)

    def spread_rows(c):
        row = pl.multiple_of(c * tall, 8)
        columns = [
            flipped[pl.ds(pl.multiple_of(4 * c * tall, 8) + m, tall, stride=4), :]
            for m in range(4)
        ]
        for i in range(levels * depth):
            for m in range(4):
                spread[i // depth, i % depth, m, pl.ds(row, tall), :] = jnp.broadcast_to(
                    columns[m][:, i : i + 1], (tall, LANES)
                )

    def add_image(t, c, row, first):
        level = STEPS - t
        y0 = pl.multiple_of(row - PAD, 8)

        def plane(z, carry):
            ws = [words[level + d, z, pl.ds(y0, tall), :] for d in (-1, 0, 1)]
            for m in range(4):
                f = [
                    (((w >> (8 * m)) & 255) - 128).astype(jnp.float32)
                    * spread[level + d, z, m, pl.ds(y0, tall), :]
                    for w, d in zip(ws, (-1, 0, 1))
                ]
                term = field[1 + t, m, RADIUS + z, pl.ds(row, tall), :] * (
                    f[2] - 2.0 * f[1] + f[0]
                )
                if first:
                    image[c, m, z] = term
                else:
                    image[c, m, z] = image[c, m, z] + term
            return carry

        lax.fori_loop(0, depth, plane, 0)

    def mute(c):
        y = c * tall + lax.broadcasted_iota(jnp.int32, (tall, LANES), 0)
        across = [(y - source[1]) ** 2 + (m * LANES + lane - source[2]) ** 2 for m in range(4)]

        def plane(z, carry):
            dz = me * depth + z - source[0]
            for m in range(4):
                dist = (across[m] + dz * dz).astype(jnp.float32)
                image[c, m, z] = image[c, m, z] * (1.0 - jnp.exp(-dist / (2.0 * MUTE * MUTE)))
            return carry

        lax.fori_loop(0, depth, plane, 0)

    far = 2 * (1 - side) + core
    near = shot

    def pair_copy(c, slot):
        return pltpu.make_async_remote_copy(
            src_ref=image.at[c],
            dst_ref=from_sibling.at[slot],
            send_sem=image_send.at[slot],
            recv_sem=image_recv.at[slot],
            device_id={"shot": sibling},
            device_id_type=MESH,
        )

    sibling_far = 2 * (1 - side) + 1 - core
    far_copy = pair_copy(sibling_far, 0)
    near_copy = pair_copy(sibling, 1)
    partner_copies = [
        pltpu.make_async_remote_copy(
            src_ref=combined.at[m],
            dst_ref=from_partner.at[m],
            send_sem=image_send.at[2 + m],
            recv_sem=image_recv.at[2 + m],
            device_id={"shot": partner},
            device_id_type=MESH,
        )
        for m in range(4)
    ]

    outs = []

    def store(src, dst):
        copy = pltpu.make_async_copy(src, dst, out_sem.at[len(outs)])
        copy.start()
        outs.append(copy)

    def first_copy(n, xc):
        c, row = rows_of(n)
        return pltpu.make_async_copy(
            field.at[0, xc, pl.ds(RADIUS, depth), pl.ds(row, tall), :],
            first_hbm.at[0, :, pl.ds(pl.multiple_of(row - PAD, 8), tall), lanes(xc)],
            out_sem.at[16 + n * 4 + xc],
        )

    for t in range(STEPS):

        def task(n, carry, t=t):
            c, row = rows_of(n)
            if t in (1, 2):
                for j in range(4):
                    b = 4 * (t - 1) + j

                    @pl.when(n == j)
                    def _():
                        if b > 0:
                            end_stage(b - 1)
                        sum_copy(b).start()
                        if hello[b] is not None:
                            pl.semaphore_signal(
                                met.at[b], inc=1, device_id=hello[b], device_id_type=MESH
                            )

            inject(t, c)

            def inner(z, carry):
                update(t, c, row, z)
                return carry

            lax.fori_loop(RADIUS, depth - RADIUS, inner, 0)
            if t == 3:

                @pl.when(n == 0)
                def _():
                    far_copy.wait_recv()

                    def plane(z, carry):
                        for m in range(4):
                            combined[m, z] = image[far, m, z] + from_sibling[0, m, z]
                        return carry

                    lax.fori_loop(0, depth, plane, 0)
                    for copy in partner_copies:
                        copy.start()

            @pl.when(has_down)
            def _():
                halo_copy(t, n, 0).wait_recv()

            lax.fori_loop(0, RADIUS, inner, 0)
            if t < STEPS - 1:

                @pl.when(has_down)
                def _():
                    halo_copy(t + 1, n, 1).start()

            @pl.when(has_up)
            def _():
                halo_copy(t, n, 1).wait_recv()

            lax.fori_loop(depth - RADIUS, depth, inner, 0)
            if t < STEPS - 1:

                @pl.when(has_up)
                def _():
                    halo_copy(t + 1, n, 0).start()

            if t == 0:
                for j in range(1, STEPS):

                    @pl.when(n == j - 1)
                    def _():
                        residuals(j)

            if t == 1:
                spread_rows(c)
                add_image(0, c, row, True)
                add_image(1, c, row, False)
            if t == 2:
                add_image(2, c, row, False)
                add_image(3, c, row, False)
            if t == STEPS - 1:
                for xc in range(4):
                    first_copy(n, xc).start()
            if t == 2:
                mute(c)

                @pl.when(c == sibling_far)
                def _():
                    far_copy.start()

                @pl.when(c == sibling)
                def _():
                    near_copy.start()

            return carry

        lax.fori_loop(0, CHUNKS, task, 0)
        if t == 2:
            last = len(stages) - 1
            end_stage(last)

            def place(k, carry):
                ordered[pl.ds((me + space_size - k) % space_size, 1)] = gathered[pl.ds(k, 1)]
                return carry

            lax.fori_loop(0, space_size, place, 0)
            everyone = jnp.sum(ordered[...], axis=0) * scale
            sums[3] = jnp.broadcast_to(everyone, sums.shape[1:])
        if t == 2:
            for xc in range(4):
                store(
                    field.at[STEPS, xc, pl.ds(RADIUS, depth), pl.ds(PAD, height), :],
                    second_hbm.at[0, :, :, lanes(xc)],
                )
            store(sums.at[3], misfit_hbm)
    near_copy.wait_recv()
    for m in range(4):
        partner_copies[m].wait_recv()

        def plane(z, carry, m=m):
            grad_out[m, z] = image[near, m, z] + from_sibling[1, m, z] + from_partner[m, z]
            return carry

        lax.fori_loop(0, depth, plane, 0)
        store(grad_out.at[m], grad_hbm.at[:, :, lanes(m)])

    def drain(n, carry):
        for t in range(STEPS):

            @pl.when(has_up)
            def _():
                halo_copy(t, n, 0).wait_send()

            @pl.when(has_down)
            def _():
                halo_copy(t, n, 1).wait_send()

        for xc in range(4):
            first_copy(n, xc).wait()
        return carry

    far_copy.wait_send()
    near_copy.wait_send()
    for copy in partner_copies:
        copy.wait_send()
    for b in range(len(stages)):
        sum_copy(b).wait_send()
    lax.fori_loop(0, CHUNKS, drain, 0)
    for copy in outs:
        copy.wait()


def finish(g_in, f_in, s_in, m_in, g_out, f_out, s_out, m_out, tile, one, sem):
    quarter = f_in.shape[1] // 4
    pairs = [(m_in, tile), (g_in, g_out)] + [
        (a.at[0, pl.ds(i * quarter, quarter)], b.at[0, pl.ds(i * quarter, quarter)])
        for a, b in ((f_in, f_out), (s_in, s_out))
        for i in range(4)
    ]
    copies = [pltpu.make_async_copy(a, b, sem.at[i]) for i, (a, b) in enumerate(pairs)]
    for copy in copies:
        copy.start()
    copies[0].wait()
    one[...] = tile[0:1, 0:1]
    last = pltpu.make_async_copy(one, m_out, sem.at[len(pairs)])
    last.start()
    for copy in copies[1:]:
        copy.wait()
    last.wait()


def body(
    space_size,
    shot_size,
    adjoint_now,
    adjoint_later,
    courant,
    checkpoint_codes,
    scale_index,
    scale_table,
    receiver_cell,
    observed,
    source_cell,
):
    _, depth, height, width = adjoint_now.shape
    levels = checkpoint_codes.shape[1]
    receivers = receiver_cell.shape[1]
    tall = height // CHUNKS
    quarter = (4, depth, tall, LANES)
    stages = (space_size * shot_size).bit_length() - 1
    whole = pl.BlockSpec(memory_space=pl.ANY)
    outside = pl.BlockSpec(memory_space=pltpu.HBM)
    f32 = jnp.float32
    results = pl.pallas_call(
        functools.partial(kernel, space_size, shot_size),
        out_shape=(
            jax.ShapeDtypeStruct((depth, tall, width), f32),
            jax.ShapeDtypeStruct(adjoint_now.shape, f32),
            jax.ShapeDtypeStruct(adjoint_now.shape, f32),
            jax.ShapeDtypeStruct((8, LANES), f32),
        ),
        in_specs=[outside] * 9,
        out_specs=[whole] * 4,
        scratch_shapes=[
            pltpu.SMEM(scale_table.shape, f32),
            pltpu.SMEM(source_cell.shape, jnp.int32),
            pltpu.VMEM((STEPS + 1, 4, depth + 2 * RADIUS, height + 2 * PAD, LANES), f32),
            pltpu.VMEM((4, depth, height, LANES), f32),
            pltpu.VMEM((levels, depth, height, LANES), jnp.int32),
            pltpu.VMEM((levels, depth, 4 * height), jnp.int32),
            pltpu.VMEM((1, receivers), jnp.int32),
            pltpu.VMEM((STEPS, receivers), f32),
            pltpu.VMEM((LANES, 4 * height), f32),
            pltpu.VMEM((4 * height, LANES), f32),
            pltpu.VMEM((levels, depth, 4, height, LANES), f32),
            pltpu.VMEM((depth, height, receivers), jnp.bfloat16),
            pltpu.VMEM((width, receivers), jnp.bfloat16),
            pltpu.VMEM((STEPS, 3, width, receivers), jnp.bfloat16),
            pltpu.VMEM(quarter, f32),
            pltpu.VMEM((LANES, receivers), f32),
            pltpu.VMEM((CHUNKS, *quarter), f32),
            pltpu.VMEM((2, *quarter), f32),
            pltpu.VMEM(quarter, f32),
            pltpu.VMEM(quarter, f32),
            pltpu.VMEM(quarter, f32),
            pltpu.VMEM((4, 8, LANES), f32),
            pltpu.VMEM((2, 8, LANES), f32),
            pltpu.VMEM((space_size, 1, LANES), f32),
            pltpu.VMEM((space_size, 1, LANES), f32),
            pltpu.SemaphoreType.DMA((32,)),
            pltpu.SemaphoreType.DMA((32,)),
            pltpu.SemaphoreType.DMA((2, STEPS, CHUNKS)),
            pltpu.SemaphoreType.DMA((2, STEPS, CHUNKS)),
            pltpu.SemaphoreType.DMA((6,)),
            pltpu.SemaphoreType.DMA((6,)),
            pltpu.SemaphoreType.DMA((stages,)),
            pltpu.SemaphoreType.DMA((stages,)),
            pltpu.SemaphoreType.REGULAR((stages,)),
        ],
        compiler_params=pltpu.CompilerParams(
            collective_id=0, has_side_effects=True, vmem_limit_bytes=48 * 1024 * 1024
        ),
    )(
        *(
            pltpu.with_memory_space_constraint(x, pltpu.HBM)
            for x in (
                adjoint_now,
                adjoint_later,
                courant,
                checkpoint_codes,
                scale_index,
                receiver_cell,
                observed,
                scale_table,
                source_cell,
            )
        )
    )
    gradient, first, second, misfit = pl.pallas_call(
        finish,
        out_shape=tuple(
            jax.ShapeDtypeStruct(x.shape if i < 3 else (1, 1), f32) for i, x in enumerate(results)
        ),
        in_specs=[whole] * 4,
        out_specs=[outside] * 4,
        scratch_shapes=[
            pltpu.VMEM((8, LANES), f32),
            pltpu.VMEM((1, 1), f32),
            pltpu.SemaphoreType.DMA((11,)),
        ],
        compiler_params=pltpu.CompilerParams(vmem_limit_bytes=1024 * 1024),
    )(*results)
    return gradient, first, second, misfit.reshape(())


def solution(mesh):
    sizes = dict(mesh.shape)
    return jax.shard_map(
        functools.partial(body, sizes["space"], sizes["shot"]),
        mesh=mesh,
        in_specs=(
            P("shot", "space", None, None),
            P("shot", "space", None, None),
            P("space", None, None),
            P("shot", None, "space", None, None),
            P("shot", None, "space", None),
            P(),
            P("shot", "space"),
            P("shot", None, "space"),
            P("shot", None),
        ),
        out_specs=(
            P("space", "shot", None),
            P("shot", "space", None, None),
            P("shot", "space", None, None),
            P(),
        ),
        check_vma=False,
    )
```
